128 devices in a mesh: layer: 4 (over x), row: 16 (over z, y), col: 2 (over core).
Axes of the slice: x: 4, y: 4, z: 4, core: 2. Of those that a mesh axis runs over, the one named last changes fastest.
Arguments:
- statistic: float32 [8, 7168, 7168], P('layer', 'row', 'col'), as said below
- eigenbasis: float32 [8, 7168, 1024], P('layer', 'col'), may hold values from -0.0625 to 0.0625
Outputs:
- refreshed: float32 [8, 7168, 1024], P('layer', ('row', 'col'))
The draws below stay inside these ranges and needn't reach their ends.
Inputs may be any that keep to these rules, and one draw needn't show every extreme that they name: `statistic`: each layer's matrix is symmetric and positive definite.
All inputs are finite; a program needn't handle non-finite values.
Results may differ from the reference program's by a relative error of at most 0.00014.
Values sent between devices are 32-bit elements; how exact they have to be, the bound alone decides.
A program may use at most 192 MiB of HBM per device.

```python
import math
import jax
import jax.numpy as jnp
from jax import lax

D = 7168
K = 1024
LAYERS = 8


def draw_statistic(key, part):
    noise_key = jax.random.fold_in(key, 11)
    diag_key = jax.random.fold_in(key, 12)
    noise_part = jax.random.normal(noise_key, (LAYERS, D, D), jnp.float32) * (0.35 / math.sqrt(D))
    symmetric = (noise_part + jnp.swapaxes(noise_part, 1, 2)) * math.sqrt(0.5)
    upper_log = math.log(3.0)
    diag_values = jnp.exp(jax.random.uniform(diag_key, (LAYERS, D), jnp.float32, 0.0, upper_log))
    return symmetric + diag_values[:, :, None] * jnp.eye(D, dtype=jnp.float32)


def levels(rng, shape, cuts, smallest, top_value):
    gain, own = 1.0, jax.random.fold_in(rng, 6)
    for axis_at, parts in cuts:
        steps = jnp.exp(jax.random.uniform(jax.random.fold_in(own, axis_at), (parts,), jnp.float32, smallest / len(cuts), top_value / len(cuts)))
        gain = gain * jnp.repeat(steps, shape[axis_at] // parts).reshape([-1 if axis == axis_at else 1 for axis in range(len(shape))])
    return gain


def bell_draw(own_key, dims, width, most, shards=(), kind=jnp.bfloat16):
    loudness = levels(own_key, dims, shards, -0.22, 0.18) if shards else 1.0
    array = jax.random.normal(own_key, dims, jnp.float32) * width * loudness
    return jnp.minimum(jnp.maximum(array, -most), most).astype(kind)


def setup_inputs(seed: int = 0) -> dict:
    streams_of = jax.random.split(jax.random.key(seed), 3)
    statistic = draw_statistic(jax.random.fold_in(streams_of[2], 71), 0)
    eigenbasis = bell_draw(streams_of[1], (LAYERS, D, K), D ** -0.5, 0.0625, ((0, 4), (1, 2)), jnp.float32)
    return dict(statistic=statistic, eigenbasis=eigenbasis)


def refresh_layer(operands):
    stat_layer, basis_layer = operands
    product = jnp.dot(stat_layer.astype(jnp.float32), basis_layer.astype(jnp.float32), precision=lax.Precision.HIGHEST, preferred_element_type=jnp.float32)
    gram_matrix = lax.dot_general(product.astype(jnp.float32), product.astype(jnp.float32), (((0,), (0,)), ((), ())), precision=lax.Precision.HIGHEST, preferred_element_type=jnp.float32)
    factor = jnp.linalg.cholesky(gram_matrix)
    return lax.linalg.triangular_solve(factor, product, left_side=False, lower=True, transpose_a=True)

def reference(statistic, eigenbasis):
    return lax.map(refresh_layer, (statistic, eigenbasis))
```

```python
import functools
import jax, jax.numpy as jnp
from jax import lax
from jax.experimental import pallas as pl
from jax.experimental.pallas import tpu as pltpu
from jax.sharding import PartitionSpec as P

F32, BF16 = jnp.float32, jnp.bfloat16

def halves(x):
    hi = x.astype(BF16)
    lo = (x - hi.astype(F32)).astype(BF16)
    return hi, lo

def left_stack(x):
    hi, lo = halves(x)
    return jnp.concatenate([hi, lo, hi, lo], axis=1)

def right_stack(x):
    hi, lo = halves(x)
    return jnp.concatenate([hi, hi, lo, lo], axis=0)

def dot(a, b):
    return jnp.dot(a, b, preferred_element_type=F32)

def factor_group(rows, inv, col0):
    n = len(rows)
    sub = lax.broadcasted_iota(jnp.int32, (8, 128), 0)
    for t in range(n):
        base = col0 + 8 * t
        cols = [[jnp.broadcast_to(rows[g][:, base + j:base + j + 1], (8, 128)) for g in range(t, n)] for j in range(8)]
        scale = None
        for j in range(8):
            pivot = jnp.broadcast_to(cols[j][0][j:j + 1, :], (8, 128))
            recip = 1.0 / pivot
            rs = lax.rsqrt(pivot)
            scale = rs if scale is None else jnp.where(sub >= j, rs, scale)
            mult = [c * recip for c in cols[j]]
            mult[0] = jnp.where(sub > j, mult[0], 0.0)
            for k in range(j + 1, 8):
                across = jnp.broadcast_to(cols[k][0][j:j + 1, :], (8, 128))
                cols[k] = [c - m * across for c, m in zip(cols[k], mult)]
            row = jnp.broadcast_to(rows[t][j:j + 1, :], (8, 128))
            irow = jnp.broadcast_to(inv[t][j:j + 1, :], (8, 128))
            for g in range(t, n):
                rows[g] = rows[g] - mult[g - t] * row
                inv[g] = inv[g] - mult[g - t] * irow
        rows[t] = rows[t] * scale
        inv[t] = inv[t] * scale
    return rows, inv

def diag_inverse(load, work, winv):
    r = lax.broadcasted_iota(jnp.int32, (128, 128), 0)
    c = lax.broadcasted_iota(jnp.int32, (128, 128), 1)
    work[...] = load
    winv[...] = jnp.where(r == c, 1.0, 0.0).astype(F32)
    step = 32
    for q in range(128 // step):
        lo = q * step
        rows = [work[lo + 8 * g:lo + 8 * g + 8, :] for g in range(step // 8)]
        inv = [winv[lo + 8 * g:lo + 8 * g + 8, :] for g in range(step // 8)]
        rows, inv = factor_group(rows, inv, lo)
        rfull = jnp.concatenate(rows, axis=0)
        ifull = jnp.concatenate(inv, axis=0)
        winv[lo:lo + step, :] = ifull
        if lo + step < 128:
            both = right_stack(jnp.concatenate([rfull, ifull], axis=1))
            lt = left_stack(rfull.T)
            upd = dot(lt[lo + step:, :], both)
            work[lo + step:, :] -= upd[:, :128]
            winv[lo + step:, :] -= upd[:, 128:]

def kernel(n, g_ref, p_ref, x_ref, G, work, winv, Rr):
    G[...] = g_ref[...]
    x_ref[...] = p_ref[...]

    def body(k, carry):
        at = pl.multiple_of(k * 128, 128)
        diag_inverse(G[pl.ds(at, 128), pl.ds(at, 128)], work, winv)
        m = winv[...]
        ml = left_stack(m)
        mt = right_stack(m.T)
        for kk in range(n):
            @pl.when(k == kk)
            def _():
                a = kk * 128
                b = a + 128
                xk = dot(left_stack(x_ref[:, a:b]), mt)
                x_ref[:, a:b] = xk
                if kk < n - 1:
                    r = dot(ml, right_stack(G[a:b, b:]))
                    rr = right_stack(r)
                    x_ref[:, b:] -= dot(left_stack(xk), rr)
                    w = n * 128 - b
                    for i in range(0, w, 256):
                        e = min(i + 256, w)
                        lt = left_stack(r[:, i:e].T)
                        G[b + i:b + e, b + i:] -= dot(lt, rr[:, i:])
        return carry
    lax.fori_loop(0, n, body, 0)

def chol_solve(gram, prod):
    k = gram.shape[0]
    n = k // 128
    vm = pl.BlockSpec(memory_space=pltpu.VMEM)
    return pl.pallas_call(
        functools.partial(kernel, n),
        out_shape=jax.ShapeDtypeStruct(prod.shape, F32),
        in_specs=[vm, vm],
        out_specs=vm,
        scratch_shapes=[pltpu.VMEM((k, k), F32), pltpu.VMEM((128, 128), F32), pltpu.VMEM((128, 128), F32), pltpu.VMEM((8, 128), F32)],
        compiler_params=pltpu.CompilerParams(vmem_limit_bytes=48 << 20),
        name="chol_solve",
    )(gram, prod)


HIGH = lax.Precision.HIGH


def on_device(statistic, eigenbasis):
    partial = jnp.stack(
        [jnp.dot(statistic[l], eigenbasis[l], precision=HIGH, preferred_element_type=F32) for l in range(2)]
    )
    product = lax.psum_scatter(partial, "col", scatter_dimension=0, tiled=False)
    gram = lax.dot_general(product, product, (((0,), (0,)), ((), ())), precision=HIGH, preferred_element_type=F32)
    gram = lax.psum(gram, "row")
    x = chol_solve(gram, product)
    x = x.reshape(2, x.shape[0] // 2, x.shape[1])
    return lax.all_to_all(x, "col", 0, 0)


def solution(mesh):
    placed = (P("layer", "row", "col"), P("layer", "col", None))
    return jax.shard_map(
        on_device,
        mesh=mesh,
        in_specs=placed,
        out_specs=P("layer", ("row", "col"), None),
        check_vma=False,
    )
```

```python
import functools
import jax
import jax.numpy as jnp
from jax import lax
from jax.experimental import pallas as pl
from jax.experimental.pallas import tpu as pltpu
from jax.sharding import PartitionSpec as P

F32, BF16 = jnp.float32, jnp.bfloat16
MESH = pl.DeviceIdType.MESH
HIGH = lax.Precision.HIGH
B = 128


def halves(x):
    hi = x.astype(BF16)
    lo = (x - hi.astype(F32)).astype(BF16)
    return hi, lo


def dot(a, b):
    return jnp.dot(a, b, preferred_element_type=F32)


def dot_t(a, b):
    return lax.dot_general(a, b, (((1,), (1,)), ((), ())), preferred_element_type=F32)


def left_stack(x):
    hi, lo = halves(x)
    return jnp.concatenate([hi, lo, hi, lo], axis=1)


def right_stack(x):
    hi, lo = halves(x)
    return jnp.concatenate([hi, hi, lo, lo], axis=0)


def factor_group(rows, inv, col0):
    n = len(rows)
    sub = lax.broadcasted_iota(jnp.int32, (8, 128), 0)
    for t in range(n):
        base = col0 + 8 * t
        cols = [
            [jnp.broadcast_to(rows[g][:, base + j : base + j + 1], (8, 128)) for g in range(t, n)]
            for j in range(8)
        ]
        scale = None
        for j in range(8):
            pivot = jnp.broadcast_to(cols[j][0][j : j + 1, :], (8, 128))
            recip = 1.0 / pivot
            rs = lax.rsqrt(pivot)
            scale = rs if scale is None else jnp.where(sub >= j, rs, scale)
            mult = [c * recip for c in cols[j]]
            mult[0] = jnp.where(sub > j, mult[0], 0.0)
            for k in range(j + 1, 8):
                across = jnp.broadcast_to(cols[k][0][j : j + 1, :], (8, 128))
                cols[k] = [c - m * across for c, m in zip(cols[k], mult)]
            row = jnp.broadcast_to(rows[t][j : j + 1, :], (8, 128))
            irow = jnp.broadcast_to(inv[t][j : j + 1, :], (8, 128))
            for g in range(t, n):
                rows[g] = rows[g] - mult[g - t] * row
                inv[g] = inv[g] - mult[g - t] * irow
        rows[t] = rows[t] * scale
        inv[t] = inv[t] * scale
    return rows, inv


def diag_inverse(block, work, winv):
    r = lax.broadcasted_iota(jnp.int32, (B, B), 0)
    c = lax.broadcasted_iota(jnp.int32, (B, B), 1)
    work[...] = block
    winv[...] = jnp.where(r == c, 1.0, 0.0).astype(F32)
    step = 32
    for q in range(B // step):
        lo = q * step
        rows = [work[lo + 8 * g : lo + 8 * g + 8, :] for g in range(step // 8)]
        inv = [winv[lo + 8 * g : lo + 8 * g + 8, :] for g in range(step // 8)]
        rows, inv = factor_group(rows, inv, lo)
        rfull = jnp.concatenate(rows, axis=0)
        ifull = jnp.concatenate(inv, axis=0)
        winv[lo : lo + step, :] = ifull
        if lo + step < B:
            both = right_stack(jnp.concatenate([rfull, ifull], axis=1))
            lt = left_stack(rfull.T)
            upd = dot(lt[lo + step :, :], both)
            work[lo + step :, :] -= upd[:, :B]
            winv[lo + step :, :] -= upd[:, B:]
    return winv[...]


def panel_at(k):
    return B * k * (k + 1) // 2


def kernel(nb, part, out, pin, phi, plo, thi, tlo, gloc, gfull, ysum, r1, r2, whi, wlo, x, work, winv,
           xsend, xrecv, osend, orecv, asend, arecv):
    core = lax.axis_index("col")
    row = lax.axis_index("row")
    a, b = row // 4, row % 4
    mate = {"col": 1 - core}

    def along(first, d):
        if first:
            return a * 4 + (b + d) % 4
        return ((a + d) % 4) * 4 + b

    barrier = pltpu.get_barrier_semaphore()
    pl.semaphore_signal(barrier, inc=1, device_id=mate, device_id_type=MESH)
    for d in range(1, 4):
        pl.semaphore_signal(barrier, inc=1, device_id={"row": along(True, d)}, device_id_type=MESH)
        pl.semaphore_signal(barrier, inc=1, device_id={"row": along(False, d)}, device_id_type=MESH)
    pl.semaphore_wait(barrier, 7)

    rows = phi.shape[0]
    half = rows // 2
    sends = []

    def swap(q):
        cols = slice(256 * q, 256 * q + 256)
        return pltpu.make_async_remote_copy(
            src_ref=part.at[1 - core, :, cols], dst_ref=pin.at[:, cols],
            send_sem=xsend.at[q], recv_sem=xrecv.at[q], device_id=mate, device_id_type=MESH)

    swaps = [swap(q) for q in range(nb // 2)]
    for s in swaps:
        s.start()

    def coords(k):
        return (b, a) if k % 2 == 0 else (a, b)

    def reduce_copies(k, s):
        first = k % 2 == 0
        me1, me2 = coords(k)
        big, small = 32 * (k + 1), 8 * (k + 1)
        base = panel_at(k)
        made = []
        for d in range(1, 4):
            if s == 0:
                at = pl.multiple_of(base + ((me1 + d) % 4) * big, 8)
                src, dst = gloc.at[pl.ds(at, big)], r1.at[d - 1, pl.ds(base // 4, big)]
                peer = along(first, d)
            elif s == 1:
                at = pl.multiple_of(base // 4 + ((me2 + d) % 4) * small, 8)
                src, dst = ysum.at[pl.ds(at, small)], r2.at[d - 1, pl.ds(base // 16, small)]
                peer = along(not first, d)
            elif s == 2:
                at = pl.multiple_of(base + me1 * big + me2 * small, 8)
                src = dst = gfull.at[pl.ds(at, small)]
                peer = along(not first, d)
            else:
                at = pl.multiple_of(base + me1 * big, 8)
                src = dst = gfull.at[pl.ds(at, big)]
                peer = along(first, d)
            made.append(pltpu.make_async_remote_copy(
                src_ref=src, dst_ref=dst, send_sem=asend.at[k, s, d - 1], recv_sem=arecv.at[k, s, d - 1],
                device_id={"row": peer}, device_id_type=MESH))
        return made

    copies = {}

    def begin(k, s):
        copies[k, s] = reduce_copies(k, s)
        for c in copies[k, s]:
            c.start()

    def event(k, s):
        me1, me2 = coords(k)
        big, small = 32 * (k + 1), 8 * (k + 1)
        base = panel_at(k)
        for c in copies[k, s - 1]:
            c.wait_recv()
        if s == 1:
            at = pl.multiple_of(base + me1 * big, 8)
            here = slice(base // 4, base // 4 + big)
            ysum[here, :] = (gloc[pl.ds(at, big), :] + r1[0, here, :]) + (r1[1, here, :] + r1[2, here, :])
            begin(k, 1)
        elif s == 2:
            at = pl.multiple_of(base // 4 + me2 * small, 8)
            here = slice(base // 16, base // 16 + small)
            to = pl.multiple_of(base + me1 * big + me2 * small, 8)
            gfull[pl.ds(to, small), :] = (ysum[pl.ds(at, small), :] + r2[0, here, :]) + (r2[1, here, :] + r2[2, here, :])
            begin(k, 2)
        elif s == 3:
            begin(k, 3)

    def wave(*pairs):
        for q, s in pairs:
            event(2 * q, s)
            event(2 * q + 1, s)

    for q in range(nb // 2):
        cols = slice(256 * q, 256 * q + 256)
        swaps[q].wait_recv()
        prod = part[core, :, cols] + pin[:, cols]
        hi, lo = halves(prod)
        phi[:, cols] = hi
        plo[:, cols] = lo
        turned = prod.T
        hi_t, lo_t = halves(turned)
        thi[cols, :] = hi_t
        tlo[cols, :] = lo_t
        n = 256 * q + 256
        for i in range(0, n, 256):
            ii = slice(i, i + 256)
            g = dot(thi[ii, :], hi) + (dot(tlo[ii, :], hi) + dot(thi[ii, :], lo))
            e = panel_at(2 * q)
            o = panel_at(2 * q + 1)
            take = min(256, e + 256 * q + B - (e + i))
            gloc[e + i : e + i + take, :] = g[:take, :B]
            gloc[o + i : o + i + 256, :] = g[:, B:]
        begin(2 * q, 0)
        begin(2 * q + 1, 0)

    wave((0, 1))
    wave((0, 2), (1, 1))
    wave((0, 3), (1, 2), (2, 1))
    wave((0, 4), (1, 3), (2, 2), (3, 1))

    out_copies = []
    for k in range(nb):
        base = panel_at(k)
        n = B * k
        kk = slice(n, n + B)
        block = gfull[base + n : base + n + B, :]
        if k > 0:
            ghi, glo = halves(gfull[base : base + n, :])
            gboth = jnp.concatenate([ghi, glo], axis=1)
            parts = []
            for i in range(k):
                m = B * i + B
                ii = slice(B * i, m)
                r = dot(whi[ii, :m], gboth[:m]) + dot(wlo[ii, :m], gboth[:m])
                parts.append(r[:, :B] + r[:, B:])
            r = jnp.concatenate(parts, axis=0)
            rhi, rlo = halves(r)
            rboth = jnp.concatenate([rhi, rlo], axis=1)
            thr, tlr = halves(r.T)
            d = dot(thr, rboth) + dot(tlr, rboth)
            block = block - (d[:, :B] + d[:, B:])
        inv = diag_inverse(block, work, winv)
        ihi, ilo = halves(inv)
        whi[kk, kk] = ihi
        wlo[kk, kk] = ilo
        if k > 0:
            t = dot(thr, whi[:n, :n]) + (dot(tlr, whi[:n, :n]) + dot(thr, wlo[:n, :n]))
            w = -dot(left_stack(inv), right_stack(t))
            hi, lo = halves(w)
            whi[kk, :n] = hi
            wlo[kk, :n] = lo
        if k + 1 < nb:
            for i in range(k + 1):
                zero = jnp.zeros((B, B), BF16)
                whi[B * i : B * i + B, n + B : n + 2 * B] = zero
                wlo[B * i : B * i + B, n + B : n + 2 * B] = zero
        m = n + B
        x[:, kk] = dot_t(phi[:, :m], whi[kk, :m]) + (dot_t(plo[:, :m], whi[kk, :m]) + dot_t(phi[:, :m], wlo[kk, :m]))
        if k % 2 == 1:
            cols = slice(n - B, n + B)
            c = pltpu.make_async_remote_copy(
                src_ref=x.at[pl.ds(pl.multiple_of((1 - core) * half, 8), half), cols],
                dst_ref=out.at[core, :, cols],
                send_sem=osend.at[k // 2], recv_sem=orecv.at[k // 2], device_id=mate, device_id_type=MESH)
            c.start()
            out_copies.append(c)
            out[core, :, cols] = x[pl.ds(pl.multiple_of(core * half, 8), half), cols]
        if k == 0:
            wave((1, 4), (2, 3), (3, 2))
        elif k == 2:
            wave((2, 4), (3, 3))
        elif k == 4:
            wave((3, 4))

    for c in out_copies:
        c.wait()
    for s in swaps:
        s.wait_send()
    for made in copies.values():
        for c in made:
            c.wait_send()


def refresh(part):
    _, rows, k = part.shape
    nb = k // B
    vm = pl.BlockSpec(memory_space=pltpu.VMEM)
    total = panel_at(nb)
    dma = pltpu.SemaphoreType.DMA
    return pl.pallas_call(
        functools.partial(kernel, nb),
        out_shape=jax.ShapeDtypeStruct((2, rows // 2, k), F32),
        in_specs=[vm],
        out_specs=vm,
        scratch_shapes=[
            pltpu.VMEM((rows, k), F32),
            pltpu.VMEM((rows, k), BF16),
            pltpu.VMEM((rows, k), BF16),
            pltpu.VMEM((k, rows), BF16),
            pltpu.VMEM((k, rows), BF16),
            pltpu.VMEM((total, B), F32),
            pltpu.VMEM((total, B), F32),
            pltpu.VMEM((total // 4, B), F32),
            pltpu.VMEM((3, total // 4, B), F32),
            pltpu.VMEM((3, total // 16, B), F32),
            pltpu.VMEM((k, k), BF16),
            pltpu.VMEM((k, k), BF16),
            pltpu.VMEM((rows, k), F32),
            pltpu.VMEM((B, B), F32),
            pltpu.VMEM((B, B), F32),
            dma((nb // 2,)),
            dma((nb // 2,)),
            dma((nb // 2,)),
            dma((nb // 2,)),
            dma((nb, 4, 3)),
            dma((nb, 4, 3)),
        ],
        compiler_params=pltpu.CompilerParams(
            vmem_limit_bytes=48 << 20, collective_id=0, has_side_effects=True),
        name="refresh",
    )(part)


def on_device(statistic, eigenbasis):
    part = lax.dot_general(
        statistic, eigenbasis, (((2,), (1,)), ((0,), (0,))), precision=HIGH, preferred_element_type=F32)
    return refresh(part)


def solution(mesh):
    placed = (P("layer", "row", "col"), P("layer", "col", None))
    return jax.shard_map(
        on_device,
        mesh=mesh,
        in_specs=placed,
        out_specs=P("layer", ("row", "col"), None),
        check_vma=False,
    )
```

```python
import functools
import jax
import jax.numpy as jnp
from jax import lax
from jax.experimental import pallas as pl
from jax.experimental.pallas import tpu as pltpu
from jax.sharding import PartitionSpec as P

F32, BF16 = jnp.float32, jnp.bfloat16
MESH = pl.DeviceIdType.MESH
B = 128
KC = 512


def halves(x):
    hi = x.astype(BF16)
    lo = (x - hi.astype(F32)).astype(BF16)
    return hi, lo


def dot(a, b):
    return jnp.dot(a, b, preferred_element_type=F32)


def dot_t(a, b):
    return lax.dot_general(a, b, (((1,), (1,)), ((), ())), preferred_element_type=F32)


def left_stack(x):
    hi, lo = halves(x)
    return jnp.concatenate([hi, lo, hi, lo], axis=1)


def right_stack(x):
    hi, lo = halves(x)
    return jnp.concatenate([hi, hi, lo, lo], axis=0)


def factor_group(rows, inv, col0):
    n = len(rows)
    sub = lax.broadcasted_iota(jnp.int32, (8, 128), 0)
    for t in range(n):
        base = col0 + 8 * t
        cols = [
            [jnp.broadcast_to(rows[g][:, base + j : base + j + 1], (8, 128)) for g in range(t, n)]
            for j in range(8)
        ]
        scale = None
        for j in range(8):
            pivot = jnp.broadcast_to(cols[j][0][j : j + 1, :], (8, 128))
            recip = 1.0 / pivot
            rs = lax.rsqrt(pivot)
            scale = rs if scale is None else jnp.where(sub >= j, rs, scale)
            mult = [c * recip for c in cols[j]]
            mult[0] = jnp.where(sub > j, mult[0], 0.0)
            for k in range(j + 1, 8):
                across = jnp.broadcast_to(cols[k][0][j : j + 1, :], (8, 128))
                cols[k] = [c - m * across for c, m in zip(cols[k], mult)]
            row = jnp.broadcast_to(rows[t][j : j + 1, :], (8, 128))
            irow = jnp.broadcast_to(inv[t][j : j + 1, :], (8, 128))
            for g in range(t, n):
                rows[g] = rows[g] - mult[g - t] * row
                inv[g] = inv[g] - mult[g - t] * irow
        rows[t] = rows[t] * scale
        inv[t] = inv[t] * scale
    return rows, inv


def diag_inverse(block, work, winv):
    r = lax.broadcasted_iota(jnp.int32, (B, B), 0)
    c = lax.broadcasted_iota(jnp.int32, (B, B), 1)
    work[...] = block
    winv[...] = jnp.where(r == c, 1.0, 0.0).astype(F32)
    step = 32
    for q in range(B // step):
        lo = q * step
        rows = [work[lo + 8 * g : lo + 8 * g + 8, :] for g in range(step // 8)]
        inv = [winv[lo + 8 * g : lo + 8 * g + 8, :] for g in range(step // 8)]
        rows, inv = factor_group(rows, inv, lo)
        rfull = jnp.concatenate(rows, axis=0)
        ifull = jnp.concatenate(inv, axis=0)
        winv[lo : lo + step, :] = ifull
        if lo + step < B:
            both = right_stack(jnp.concatenate([rfull, ifull], axis=1))
            lt = left_stack(rfull.T)
            upd = dot(lt[lo + step :, :], both)
            work[lo + step :, :] -= upd[:, :B]
            winv[lo + step :, :] -= upd[:, B:]
    return winv[...]


def panel_at(k):
    return B * k * (k + 1) // 2


def kernel(nb, stat, basis, out, stage, shi, slo, bbuf, pacc, pin, phi, plo, thi, tlo, gloc, gfull, ysum, r1, r2,
           whi, wlo, x, work, winv, ssem, bsem, xsend, xrecv, osend, orecv, asend, arecv):
    core = lax.axis_index("col")
    row = lax.axis_index("row")
    a, b = row // 4, row % 4
    mate = {"col": 1 - core}

    def along(first, d):
        if first:
            return a * 4 + (b + d) % 4
        return ((a + d) % 4) * 4 + b

    rows = phi.shape[0]
    half = rows // 2
    depth = basis.shape[1]
    nk = depth // KC

    def layer_of(i):
        return i * core + (1 - i) * (1 - core)

    def stat_copy(i, kc):
        ks = pl.ds(pl.multiple_of(kc * KC, 128), KC)
        return pltpu.make_async_copy(stat.at[layer_of(i), :, ks], stage.at[kc], ssem.at[kc])

    def basis_copy(i, q, kc, size):
        ks = pl.ds(pl.multiple_of(kc * size, 128), size)
        cols = pl.ds(pl.multiple_of(q * 256, 128), 256)
        return pltpu.make_async_copy(basis.at[layer_of(i), ks, cols], bbuf.at[i, ks, :], bsem.at[i, kc])

    for kc in range(nk):
        stat_copy(0, kc).start()
        basis_copy(0, 0, kc, KC).start()
    for kc in range(nk):
        basis_copy(1, 0, kc, KC).start()

    barrier = pltpu.get_barrier_semaphore()
    pl.semaphore_signal(barrier, inc=1, device_id=mate, device_id_type=MESH)
    for d in range(1, 4):
        pl.semaphore_signal(barrier, inc=1, device_id={"row": along(True, d)}, device_id_type=MESH)
        pl.semaphore_signal(barrier, inc=1, device_id={"row": along(False, d)}, device_id_type=MESH)
    pl.semaphore_wait(barrier, 7)

    def swap(q):
        return pltpu.make_async_remote_copy(
            src_ref=pacc.at[2 * q], dst_ref=pin.at[q],
            send_sem=xsend.at[q], recv_sem=xrecv.at[q], device_id=mate, device_id_type=MESH)

    def coords(k):
        return (b, a) if k % 2 == 0 else (a, b)

    def reduce_copies(k, s):
        first = k % 2 == 0
        me1, me2 = coords(k)
        big, small = 32 * (k + 1), 8 * (k + 1)
        base = panel_at(k)
        made = []
        for d in range(1, 4):
            if s == 0:
                at = pl.multiple_of(base + ((me1 + d) % 4) * big, 8)
                src, dst = gloc.at[pl.ds(at, big)], r1.at[d - 1, pl.ds(base // 4, big)]
                peer = along(first, d)
            elif s == 1:
                at = pl.multiple_of(base // 4 + ((me2 + d) % 4) * small, 8)
                src, dst = ysum.at[pl.ds(at, small)], r2.at[d - 1, pl.ds(base // 16, small)]
                peer = along(not first, d)
            elif s == 2:
                at = pl.multiple_of(base + me1 * big + me2 * small, 8)
                src = dst = gfull.at[pl.ds(at, small)]
                peer = along(not first, d)
            else:
                at = pl.multiple_of(base + me1 * big, 8)
                src = dst = gfull.at[pl.ds(at, big)]
                peer = along(first, d)
            made.append(pltpu.make_async_remote_copy(
                src_ref=src, dst_ref=dst, send_sem=asend.at[k, s, d - 1], recv_sem=arecv.at[k, s, d - 1],
                device_id={"row": peer}, device_id_type=MESH))
        return made

    def begin(k, s):
        for c in reduce_copies(k, s):
            c.start()

    def event(k, s):
        me1, me2 = coords(k)
        big, small = 32 * (k + 1), 8 * (k + 1)
        base = panel_at(k)
        for c in reduce_copies(k, s - 1):
            c.wait_recv()
        if s == 1:
            at = pl.multiple_of(base + me1 * big, 8)
            here = slice(base // 4, base // 4 + big)
            ysum[here, :] = (gloc[pl.ds(at, big), :] + r1[0, here, :]) + (r1[1, here, :] + r1[2, here, :])
            begin(k, 1)
        elif s == 2:
            at = pl.multiple_of(base // 4 + me2 * small, 8)
            here = slice(base // 16, base // 16 + small)
            to = pl.multiple_of(base + me1 * big + me2 * small, 8)
            gfull[pl.ds(to, small), :] = (ysum[pl.ds(at, small), :] + r2[0, here, :]) + (r2[1, here, :] + r2[2, here, :])
            begin(k, 2)
        elif s == 3:
            begin(k, 3)

    def wave(*pairs):
        for q, s in pairs:
            event(2 * q, s)
            event(2 * q + 1, s)

    def gram(q):
        cols = slice(256 * q, 256 * q + 256)
        swap(q).wait_recv()
        prod = pacc[2 * q + 1] + pin[q]
        hi, lo = halves(prod)
        phi[:, cols] = hi
        plo[:, cols] = lo
        hi_t, lo_t = halves(prod.T)
        thi[cols, :] = hi_t
        tlo[cols, :] = lo_t
        e, o = panel_at(2 * q), panel_at(2 * q + 1)
        for i in range(0, 256 * q + 256, 256):
            ii = slice(i, i + 256)
            g = dot(thi[ii, :], hi) + (dot(tlo[ii, :], hi) + dot(thi[ii, :], lo))
            take = min(256, 256 * q + B - i)
            gloc[e + i : e + i + take, :] = g[:take, :B]
            gloc[o + i : o + i + 256, :] = g[:, B:]
        begin(2 * q, 0)
        begin(2 * q + 1, 0)

    for i in range(2):

        def first(kc, carry):
            stat_copy(i, kc).wait()
            basis_copy(i, 0, kc, KC).wait()
            ks = pl.ds(pl.multiple_of(kc * KC, 128), KC)
            hi, lo = halves(stage[kc])
            shi[i, :, ks] = hi
            slo[i, :, ks] = lo
            if i == 0:
                stat_copy(1, kc).start()
            bhi, blo = halves(bbuf[i, ks, :])
            r = dot(hi, bhi) + dot(lo, bhi) + dot(hi, blo)

            @pl.when(kc == 0)
            def _():
                pacc[i] = r

            @pl.when(kc > 0)
            def _():
                pacc[i] += r

            return carry

        lax.fori_loop(0, nk, first, 0)
        for kc in range(2):
            basis_copy(i, 1, kc, depth // 2).start()
        if i == 0:
            swap(0).start()
    gram(0)

    plan = {
        2: ((0, 1),), 3: ((0, 2),), 4: ((0, 3), (1, 1)), 5: ((0, 4), (1, 2)), 6: ((1, 3), (2, 1)), 7: ((1, 4), (2, 2)),
    }

    def column_step(t, carry):
        q, i = t // 2, t % 2
        for kc in range(2):
            basis_copy(i, q, kc, depth // 2).wait()
        acc = None
        for kc in range(2):
            ks = slice(kc * depth // 2, (kc + 1) * depth // 2)
            bhi, blo = halves(bbuf[i, ks, :])
            for left, right in ((shi, bhi), (slo, bhi), (shi, blo)):
                r = dot(left[i, :, ks], right)
                acc = r if acc is None else acc + r
        pacc[t] = acc

        @pl.when(t < 6)
        def _():
            for kc in range(2):
                basis_copy(i, q + 1, kc, depth // 2).start()

        for tt in range(2, 8):

            @pl.when(t == tt)
            def _():
                if tt % 2 == 0:
                    swap(tt // 2).start()
                wave(*plan[tt])
                if tt % 2 == 1:
                    gram(tt // 2)

        return carry

    lax.fori_loop(2, 8, column_step, 0)

    out_copies = []
    for k in range(nb):
        base = panel_at(k)
        n = B * k
        kk = slice(n, n + B)
        block = gfull[base + n : base + n + B, :]
        if k > 0:
            ghi, glo = halves(gfull[base : base + n, :])
            gboth = jnp.concatenate([ghi, glo], axis=1)
            parts = []
            for i in range(k):
                m = B * i + B
                ii = slice(B * i, m)
                r = dot(whi[ii, :m], gboth[:m]) + dot(wlo[ii, :m], gboth[:m])
                parts.append(r[:, :B] + r[:, B:])
            r = jnp.concatenate(parts, axis=0)
            rhi, rlo = halves(r)
            rboth = jnp.concatenate([rhi, rlo], axis=1)
            thr, tlr = halves(r.T)
            d = dot(thr, rboth) + dot(tlr, rboth)
            block = block - (d[:, :B] + d[:, B:])
        inv = diag_inverse(block, work, winv)
        ihi, ilo = halves(inv)
        whi[kk, kk] = ihi
        wlo[kk, kk] = ilo
        if k > 0:
            t = dot(thr, whi[:n, :n]) + (dot(tlr, whi[:n, :n]) + dot(thr, wlo[:n, :n]))
            w = -dot(left_stack(inv), right_stack(t))
            hi, lo = halves(w)
            whi[kk, :n] = hi
            wlo[kk, :n] = lo
        if k + 1 < nb:
            for i in range(k + 1):
                zero = jnp.zeros((B, B), BF16)
                whi[B * i : B * i + B, n + B : n + 2 * B] = zero
                wlo[B * i : B * i + B, n + B : n + 2 * B] = zero
        m = n + B
        x[:, kk] = dot_t(phi[:, :m], whi[kk, :m]) + (dot_t(plo[:, :m], whi[kk, :m]) + dot_t(phi[:, :m], wlo[kk, :m]))
        if k % 2 == 1:
            cols = slice(n - B, n + B)
            c = pltpu.make_async_remote_copy(
                src_ref=x.at[pl.ds(pl.multiple_of((1 - core) * half, 8), half), cols],
                dst_ref=out.at[core, :, cols],
                send_sem=osend.at[k // 2], recv_sem=orecv.at[k // 2], device_id=mate, device_id_type=MESH)
            c.start()
            out_copies.append(c)
            out[core, :, cols] = x[pl.ds(pl.multiple_of(core * half, 8), half), cols]
        wave(*{0: ((2, 3),), 1: ((2, 4), (3, 1)), 2: ((3, 2),), 3: ((3, 3),), 5: ((3, 4),)}.get(k, ()))

    for c in out_copies:
        c.wait()
    for q in range(nb // 2):
        swap(q).wait_send()
    for k in range(nb):
        for s in range(4):
            for c in reduce_copies(k, s):
                c.wait_send()


def refresh(statistic, eigenbasis):
    _, rows, depth = statistic.shape
    k = eigenbasis.shape[2]
    nb = k // B
    vm = pl.BlockSpec(memory_space=pltpu.VMEM)
    total = panel_at(nb)
    dma = pltpu.SemaphoreType.DMA
    return pl.pallas_call(
        functools.partial(kernel, nb),
        out_shape=jax.ShapeDtypeStruct((2, rows // 2, k), F32),
        in_specs=[pl.BlockSpec(memory_space=pl.ANY)] * 2,
        out_specs=vm,
        scratch_shapes=[
            pltpu.VMEM((depth // KC, rows, KC), F32),
            pltpu.VMEM((2, rows, depth), BF16),
            pltpu.VMEM((2, rows, depth), BF16),
            pltpu.VMEM((2, depth, 256), F32),
            pltpu.VMEM((8, rows, 256), F32),
            pltpu.VMEM((4, rows, 256), F32),
            pltpu.VMEM((rows, k), BF16),
            pltpu.VMEM((rows, k), BF16),
            pltpu.VMEM((k, rows), BF16),
            pltpu.VMEM((k, rows), BF16),
            pltpu.VMEM((total, B), F32),
            pltpu.VMEM((total, B), F32),
            pltpu.VMEM((total // 4, B), F32),
            pltpu.VMEM((3, total // 4, B), F32),
            pltpu.VMEM((3, total // 16, B), F32),
            pltpu.VMEM((k, k), BF16),
            pltpu.VMEM((k, k), BF16),
            pltpu.VMEM((rows, k), F32),
            pltpu.VMEM((B, B), F32),
            pltpu.VMEM((B, B), F32),
            dma((depth // KC,)),
            dma((2, depth // KC)),
            dma((nb // 2,)),
            dma((nb // 2,)),
            dma((nb // 2,)),
            dma((nb // 2,)),
            dma((nb, 4, 3)),
            dma((nb, 4, 3)),
        ],
        compiler_params=pltpu.CompilerParams(
            vmem_limit_bytes=67043328, collective_id=0, has_side_effects=True),
        name="refresh",
    )(statistic, eigenbasis)


def solution(mesh):
    placed = (P("layer", "row", "col"), P("layer", "col", None))
    return jax.shard_map(
        refresh,
        mesh=mesh,
        in_specs=placed,
        out_specs=P("layer", ("row", "col"), None),
        check_vma=False,
    )
```

```python
import functools
import jax
import jax.numpy as jnp
from jax import lax
from jax.experimental import pallas as pl
from jax.experimental.pallas import tpu as pltpu
from jax.sharding import PartitionSpec as P

F32, BF16 = jnp.float32, jnp.bfloat16
MESH = pl.DeviceIdType.MESH
B = 128
KC = 512


def halves(x):
    hi = x.astype(BF16)
    lo = (x - hi.astype(F32)).astype(BF16)
    return hi, lo


def dot(a, b):
    return jnp.dot(a, b, preferred_element_type=F32)


def dot_t(a, b):
    return lax.dot_general(a, b, (((1,), (1,)), ((), ())), preferred_element_type=F32)


def left_stack(x):
    hi, lo = halves(x)
    return jnp.concatenate([hi, lo, hi, lo], axis=1)


def right_stack(x):
    hi, lo = halves(x)
    return jnp.concatenate([hi, hi, lo, lo], axis=0)


def spread(v, s):
    return jnp.broadcast_to(v[s : s + 1, :], (8, 128))


def factor_group(rows, inv, col0, wide):
    n = len(rows)
    sub = lax.broadcasted_iota(jnp.int32, (8, 128), 0)
    for t in range(0, n, wide // 8):
        base = col0 + 8 * t
        cols = []
        for j in range(wide):
            col = {}
            for g in range(t + j // 8, n):
                c = jnp.broadcast_to(rows[g][:, base + j : base + j + 1], (8, 128))
                col[g] = c + 0.0 if g < t + wide // 8 else c
            cols.append(col)
        pivot = spread(cols[0][t], 0)
        scale = None
        for j in range(wide):
            gj, s = t + j // 8, j % 8
            mult = {g: c / pivot for g, c in cols[j].items()}
            across = {k: spread(cols[j][t + k // 8], k % 8) for k in range(j + 1, wide)}
            rs = lax.rsqrt(pivot)
            scale = rs if s == 0 else jnp.where(sub >= s, rs, scale)
            if j + 1 < wide:
                own = spread(cols[j + 1][t + (j + 1) // 8], (j + 1) % 8)
                pivot = own - (across[j + 1] * across[j + 1]) / pivot
            for k in range(j + 1, wide):
                for g in cols[k]:
                    cols[k][g] = cols[k][g] - mult[g] * across[k]
            mult[gj] = jnp.where(sub > s, mult[gj], 0.0)
            row, irow = spread(rows[gj], s), spread(inv[gj], s)
            for g in mult:
                rows[g] = rows[g] - mult[g] * row
                inv[g] = inv[g] - mult[g] * irow
            if s == 7:
                rows[gj] = rows[gj] * scale
                inv[gj] = inv[gj] * scale
    return rows, inv


def diag_inverse(block, work, winv, step=64, wide=16):
    r = lax.broadcasted_iota(jnp.int32, (B, B), 0)
    c = lax.broadcasted_iota(jnp.int32, (B, B), 1)
    work[...] = block
    winv[...] = jnp.where(r == c, 1.0, 0.0).astype(F32)
    for lo in range(0, B, step):
        rows = [work[lo + 8 * g : lo + 8 * g + 8, :] for g in range(step // 8)]
        inv = [winv[lo + 8 * g : lo + 8 * g + 8, :] for g in range(step // 8)]
        rows, inv = factor_group(rows, inv, lo, wide)
        rfull = jnp.concatenate(rows, axis=0)
        ifull = jnp.concatenate(inv, axis=0)
        winv[lo : lo + step, :] = ifull
        if lo + step < B:
            both = right_stack(jnp.concatenate([rfull, ifull], axis=1))
            lt = left_stack(rfull.T)
            upd = dot(lt[lo + step :, :], both)
            work[lo + step :, :] -= upd[:, :B]
            winv[lo + step :, :] -= upd[:, B:]
    return winv[...]


def panel_at(k):
    return B * k * (k + 1) // 2


def kernel(nb, stat, basis, out, stage, shi, slo, bbuf, pacc, pin, phi, plo, thi, tlo, gloc, gfull, ysum, rh, r1, r2,
           whi, wlo, x, work, winv, ssem, bsem, xsend, xrecv, osend, orecv, asend, arecv):
    core = lax.axis_index("col")
    row = lax.axis_index("row")
    a, b = row // 4, row % 4
    mate = {"col": 1 - core}

    def along(first, d):
        if first:
            return a * 4 + (b + d) % 4
        return ((a + d) % 4) * 4 + b

    rows = phi.shape[0]
    half = rows // 2
    depth = basis.shape[1]
    nk = depth // KC

    def layer_of(i):
        return i * core + (1 - i) * (1 - core)

    def stat_copy(i, kc):
        ks = pl.ds(pl.multiple_of(kc * KC, 128), KC)
        return pltpu.make_async_copy(stat.at[layer_of(i), :, ks], stage.at[kc], ssem.at[kc])

    def basis_copy(i, q, kc, size):
        ks = pl.ds(pl.multiple_of(kc * size, 128), size)
        cols = pl.ds(pl.multiple_of(q * 256, 128), 256)
        return pltpu.make_async_copy(basis.at[layer_of(i), ks, cols], bbuf.at[i, ks, :], bsem.at[i, kc])

    for kc in range(nk):
        stat_copy(0, kc).start()
        basis_copy(0, 0, kc, KC).start()
    for kc in range(nk):
        basis_copy(1, 0, kc, KC).start()

    barrier = pltpu.get_barrier_semaphore()
    pl.semaphore_signal(barrier, inc=1, device_id=mate, device_id_type=MESH)
    for d in range(1, 4):
        pl.semaphore_signal(barrier, inc=1, device_id={"row": along(True, d)}, device_id_type=MESH)
        pl.semaphore_signal(barrier, inc=1, device_id={"row": along(False, d)}, device_id_type=MESH)
    pl.semaphore_wait(barrier, 7)

    def swap(q):
        return pltpu.make_async_remote_copy(
            src_ref=pacc.at[2 * q], dst_ref=pin.at[q],
            send_sem=xsend.at[q], recv_sem=xrecv.at[q], device_id=mate, device_id_type=MESH)

    def coords(k):
        return (b, a) if k % 2 == 0 else (a, b)

    def reduce_copies(k, s):
        first = k % 2 == 0
        me1, me2 = coords(k)
        big, small = 32 * (k + 1), 8 * (k + 1)
        part = big // 2
        base = panel_at(k)

        def rows_of(chunk, size, shift=0):
            return pl.ds(pl.multiple_of(base + chunk % 4 * big + shift, 8), size)

        made = []

        def add(src, dst, peer):
            d = len(made)
            made.append(pltpu.make_async_remote_copy(
                src_ref=src, dst_ref=dst, send_sem=asend.at[k, s, d], recv_sem=arecv.at[k, s, d],
                device_id={"row": peer}, device_id_type=MESH))

        if s in (2, 3):
            for d in range(1, 4):
                if s == 2:
                    at = pl.multiple_of(base // 4 + ((me2 + d) % 4) * small, 8)
                    src, dst = ysum.at[pl.ds(at, small)], r2.at[d - 1, pl.ds(base // 16, small)]
                else:
                    at = pl.multiple_of(base + me1 * big + me2 * small, 8)
                    src = dst = gfull.at[pl.ds(at, small)]
                add(src, dst, along(not first, d))
            return made
        for way, d in enumerate((1, 3)):
            if s == 0:
                src = gloc.at[rows_of(me1 + 2, part, way * part)]
                dst = rh.at[way, pl.ds(base // 8, part)]
            elif s == 1:
                src = gloc.at[rows_of(me1 + d, big)]
                dst = r1.at[way, pl.ds(base // 4, big)]
            elif s == 4:
                src = dst = gfull.at[rows_of(me1, big)]
            else:
                src = dst = gfull.at[rows_of(me1 + 4 - d, part, way * part)]
            add(src, dst, along(first, d))
        return made

    def begin(k, s):
        for c in reduce_copies(k, s):
            c.start()

    def event(k, s):
        me1, me2 = coords(k)
        big, small = 32 * (k + 1), 8 * (k + 1)
        base = panel_at(k)
        for c in reduce_copies(k, s - 1):
            c.wait_recv()
        if s == 1:
            part = big // 2
            for way, d in enumerate((1, 3)):
                at = pl.multiple_of(base + (me1 + d) % 4 * big + way * part, 8)
                gloc[pl.ds(at, part), :] += rh[way, base // 8 : base // 8 + part, :]
        elif s == 2:
            at = pl.multiple_of(base + me1 * big, 8)
            here = slice(base // 4, base // 4 + big)
            ysum[here, :] = gloc[pl.ds(at, big), :] + (r1[0, here, :] + r1[1, here, :])
        elif s == 3:
            at = pl.multiple_of(base // 4 + me2 * small, 8)
            here = slice(base // 16, base // 16 + small)
            to = pl.multiple_of(base + me1 * big + me2 * small, 8)
            gfull[pl.ds(to, small), :] = (ysum[pl.ds(at, small), :] + r2[0, here, :]) + (r2[1, here, :] + r2[2, here, :])
        if s < 6:
            begin(k, s)

    def wave(*pairs):
        for q, s in pairs:
            event(2 * q, s)
            event(2 * q + 1, s)

    def gram(q):
        cols = slice(256 * q, 256 * q + 256)
        swap(q).wait_recv()
        prod = pacc[2 * q + 1] + pin[q]
        hi, lo = halves(prod)
        phi[:, cols] = hi
        plo[:, cols] = lo
        hi_t, lo_t = halves(prod.T)
        thi[cols, :] = hi_t
        tlo[cols, :] = lo_t
        e, o = panel_at(2 * q), panel_at(2 * q + 1)
        for i in range(0, 256 * q + 256, 256):
            ii = slice(i, i + 256)
            g = dot(thi[ii, :], hi) + (dot(tlo[ii, :], hi) + dot(thi[ii, :], lo))
            take = min(256, 256 * q + B - i)
            gloc[e + i : e + i + take, :] = g[:take, :B]
            gloc[o + i : o + i + 256, :] = g[:, B:]
        begin(2 * q, 0)
        begin(2 * q + 1, 0)

    for i in range(2):

        def first(kc, carry):
            stat_copy(i, kc).wait()
            basis_copy(i, 0, kc, KC).wait()
            ks = pl.ds(pl.multiple_of(kc * KC, 128), KC)
            hi, lo = halves(stage[kc])
            shi[i, :, ks] = hi
            slo[i, :, ks] = lo
            if i == 0:
                stat_copy(1, kc).start()
            bhi, blo = halves(bbuf[i, ks, :])
            r = dot(hi, bhi) + dot(lo, bhi) + dot(hi, blo)

            @pl.when(kc == 0)
            def _():
                pacc[i] = r

            @pl.when(kc > 0)
            def _():
                pacc[i] += r

            return carry

        lax.fori_loop(0, nk, first, 0)
        for kc in range(2):
            basis_copy(i, 1, kc, depth // 2).start()
        if i == 0:
            swap(0).start()
    gram(0)

    plan = {
        2: ((0, 1),), 3: ((0, 2),), 4: ((0, 3), (1, 1)), 5: ((0, 4), (1, 2)),
        6: ((0, 5), (1, 3), (2, 1)), 7: ((0, 6), (1, 4), (2, 2)),
    }

    def column_step(t, carry):
        q, i = t // 2, t % 2
        for kc in range(2):
            basis_copy(i, q, kc, depth // 2).wait()
        acc = None
        for kc in range(2):
            ks = slice(kc * depth // 2, (kc + 1) * depth // 2)
            bhi, blo = halves(bbuf[i, ks, :])
            for left, right in ((shi, bhi), (slo, bhi), (shi, blo)):
                r = dot(left[i, :, ks], right)
                acc = r if acc is None else acc + r
        pacc[t] = acc

        @pl.when(t < 6)
        def _():
            for kc in range(2):
                basis_copy(i, q + 1, kc, depth // 2).start()

        for tt in range(2, 8):

            @pl.when(t == tt)
            def _():
                if tt % 2 == 0:
                    swap(tt // 2).start()
                wave(*plan[tt])
                if tt % 2 == 1:
                    gram(tt // 2)

        return carry

    lax.fori_loop(2, 8, column_step, 0)

    late = {
        0: ((1, 5), (2, 3), (3, 1)), 1: ((1, 6), (2, 4), (3, 2)), 2: ((2, 5), (3, 3)), 3: ((2, 6), (3, 4)),
        4: ((3, 5),), 5: ((3, 6),),
    }
    out_copies = []
    for k in range(nb):
        base = panel_at(k)
        n = B * k
        kk = slice(n, n + B)
        block = gfull[base + n : base + n + B, :]
        if k > 0:
            ghi, glo = halves(gfull[base : base + n, :])
            gboth = jnp.concatenate([ghi, glo], axis=1)
            parts = []
            for i in range(k):
                m = B * i + B
                ii = slice(B * i, m)
                r = dot(whi[ii, :m], gboth[:m]) + dot(wlo[ii, :m], gboth[:m])
                parts.append(r[:, :B] + r[:, B:])
            r = jnp.concatenate(parts, axis=0)
            rhi, rlo = halves(r)
            rboth = jnp.concatenate([rhi, rlo], axis=1)
            thr, tlr = halves(r.T)
            d = dot(thr, rboth) + dot(tlr, rboth)
            block = block - (d[:, :B] + d[:, B:])
        inv = diag_inverse(block, work, winv)
        ihi, ilo = halves(inv)
        whi[kk, kk] = ihi
        wlo[kk, kk] = ilo
        if k > 0:
            t = dot(thr, whi[:n, :n]) + (dot(tlr, whi[:n, :n]) + dot(thr, wlo[:n, :n]))
            w = -dot(left_stack(inv), right_stack(t))
            hi, lo = halves(w)
            whi[kk, :n] = hi
            wlo[kk, :n] = lo
        if k + 1 < nb:
            for i in range(k + 1):
                zero = jnp.zeros((B, B), BF16)
                whi[B * i : B * i + B, n + B : n + 2 * B] = zero
                wlo[B * i : B * i + B, n + B : n + 2 * B] = zero
        m = n + B
        x[:, kk] = dot_t(phi[:, :m], whi[kk, :m]) + (dot_t(plo[:, :m], whi[kk, :m]) + dot_t(phi[:, :m], wlo[kk, :m]))
        if k % 2 == 1:
            cols = slice(n - B, n + B)
            c = pltpu.make_async_remote_copy(
                src_ref=x.at[pl.ds(pl.multiple_of((1 - core) * half, 8), half), cols],
                dst_ref=out.at[core, :, cols],
                send_sem=osend.at[k // 2], recv_sem=orecv.at[k // 2], device_id=mate, device_id_type=MESH)
            c.start()
            out_copies.append(c)
            out[core, :, cols] = x[pl.ds(pl.multiple_of(core * half, 8), half), cols]
        wave(*late.get(k, ()))

    for c in out_copies:
        c.wait()
    for q in range(nb // 2):
        swap(q).wait_send()
    for k in range(nb):
        for s in range(6):
            for c in reduce_copies(k, s):
                c.wait_send()


def refresh(statistic, eigenbasis):
    _, rows, depth = statistic.shape
    k = eigenbasis.shape[2]
    nb = k // B
    vm = pl.BlockSpec(memory_space=pltpu.VMEM)
    total = panel_at(nb)
    dma = pltpu.SemaphoreType.DMA
    return pl.pallas_call(
        functools.partial(kernel, nb),
        out_shape=jax.ShapeDtypeStruct((2, rows // 2, k), F32),
        in_specs=[pl.BlockSpec(memory_space=pl.ANY)] * 2,
        out_specs=vm,
        scratch_shapes=[
            pltpu.VMEM((depth // KC, rows, KC), F32),
            pltpu.VMEM((2, rows, depth), BF16),
            pltpu.VMEM((2, rows, depth), BF16),
            pltpu.VMEM((2, depth, 256), F32),
            pltpu.VMEM((8, rows, 256), F32),
            pltpu.VMEM((4, rows, 256), F32),
            pltpu.VMEM((rows, k), BF16),
            pltpu.VMEM((rows, k), BF16),
            pltpu.VMEM((k, rows), BF16),
            pltpu.VMEM((k, rows), BF16),
            pltpu.VMEM((total, B), F32),
            pltpu.VMEM((total, B), F32),
            pltpu.VMEM((total // 4, B), F32),
            pltpu.VMEM((2, total // 8, B), F32),
            pltpu.VMEM((2, total // 4, B), F32),
            pltpu.VMEM((3, total // 16, B), F32),
            pltpu.VMEM((k, k), BF16),
            pltpu.VMEM((k, k), BF16),
            pltpu.VMEM((rows, k), F32),
            pltpu.VMEM((B, B), F32),
            pltpu.VMEM((B, B), F32),
            dma((depth // KC,)),
            dma((2, depth // KC)),
            dma((nb // 2,)),
            dma((nb // 2,)),
            dma((nb // 2,)),
            dma((nb // 2,)),
            dma((nb, 6, 3)),
            dma((nb, 6, 3)),
        ],
        compiler_params=pltpu.CompilerParams(
            vmem_limit_bytes=67043328, collective_id=0, has_side_effects=True),
        name="refresh",
    )(statistic, eigenbasis)


def solution(mesh):
    placed = (P("layer", "row", "col"), P("layer", "col", None))
    return jax.shard_map(
        refresh,
        mesh=mesh,
        in_specs=placed,
        out_specs=P("layer", ("row", "col"), None),
        check_vma=False,
    )
```

```python
import functools
import jax
import jax.numpy as jnp
from jax import lax
from jax.experimental import pallas as pl
from jax.experimental.pallas import tpu as pltpu
from jax.sharding import PartitionSpec as P

F32, BF16 = jnp.float32, jnp.bfloat16
MESH = pl.DeviceIdType.MESH
B = 128
KC = 512
RING = (2, 3)
LATE = (4, 6)
DIRECT_STAGES = ("all", "second", "spread2", "spread")
RING_STAGES = ("half", "whole", "second", "spread2", "near", "relay")


def stages(k):
    return RING_STAGES if k // 2 in RING else DIRECT_STAGES


def halves(x):
    hi = x.astype(BF16)
    lo = (x - hi.astype(F32)).astype(BF16)
    return hi, lo


def dot(a, b):
    return jnp.dot(a, b, preferred_element_type=F32)


def dot_t(a, b):
    return lax.dot_general(a, b, (((1,), (1,)), ((), ())), preferred_element_type=F32)


def left_stack(x):
    hi, lo = halves(x)
    return jnp.concatenate([hi, lo, hi, lo], axis=1)


def right_stack(x):
    hi, lo = halves(x)
    return jnp.concatenate([hi, hi, lo, lo], axis=0)


def spread(v, s):
    return jnp.broadcast_to(v[s : s + 1, :], (8, 128))


def factor_group(rows, inv, col0, wide, fill):
    n = len(rows)
    sub = lax.broadcasted_iota(jnp.int32, (8, 128), 0)
    for t in range(0, n, wide // 8):
        base = col0 + 8 * t
        cols = []
        for j in range(wide):
            col = {}
            for g in range(t + j // 8, n):
                c = jnp.broadcast_to(rows[g][:, base + j : base + j + 1], (8, 128))
                col[g] = c + 0.0 if g < t + wide // 8 else c
            cols.append(col)
        pivot = spread(cols[0][t], 0)
        scale = None
        for j in range(wide):
            gj, s = t + j // 8, j % 8
            mult = {g: c / pivot for g, c in cols[j].items()}
            across = {k: spread(cols[j][t + k // 8], k % 8) for k in range(j + 1, wide)}
            rs = lax.rsqrt(pivot)
            scale = rs if s == 0 else jnp.where(sub >= s, rs, scale)
            if j + 1 < wide:
                own = spread(cols[j + 1][t + (j + 1) // 8], (j + 1) % 8)
                pivot = own - (across[j + 1] * across[j + 1]) / pivot
            for k in range(j + 1, wide):
                for g in cols[k]:
                    cols[k][g] = cols[k][g] - mult[g] * across[k]
            mult[gj] = jnp.where(sub > s, mult[gj], 0.0)
            row, irow = spread(rows[gj], s), spread(inv[gj], s)
            for g in mult:
                rows[g] = rows[g] - mult[g] * row
                inv[g] = inv[g] - mult[g] * irow
            if s == 7:
                rows[gj] = rows[gj] * scale
                inv[gj] = inv[gj] * scale
            fill()
    return rows, inv


def diag_inverse(block, work, winv, fill, step=64, wide=16):
    r = lax.broadcasted_iota(jnp.int32, (B, B), 0)
    c = lax.broadcasted_iota(jnp.int32, (B, B), 1)
    work[...] = block
    winv[...] = jnp.where(r == c, 1.0, 0.0).astype(F32)
    for lo in range(0, B, step):
        rows = [work[lo + 8 * g : lo + 8 * g + 8, :] for g in range(step // 8)]
        inv = [winv[lo + 8 * g : lo + 8 * g + 8, :] for g in range(step // 8)]
        rows, inv = factor_group(rows, inv, lo, wide, fill)
        rfull = jnp.concatenate(rows, axis=0)
        ifull = jnp.concatenate(inv, axis=0)
        winv[lo : lo + step, :] = ifull
        if lo + step < B:
            both = right_stack(jnp.concatenate([rfull, ifull], axis=1))
            lt = left_stack(rfull.T)
            upd = dot(lt[lo + step :, :], both)
            work[lo + step :, :] -= upd[:, :B]
            winv[lo + step :, :] -= upd[:, B:]
    return winv[...]


def panel_at(k):
    return B * k * (k + 1) // 2


def factor_and_solve(nb, gfull, phi, plo, whi, wlo, x, work, winv, gboth, rboth, thr, tlr, tk, bd, after):
    rows = phi.shape[0]
    zero = jnp.zeros((B, B), BF16)
    for i in range(0, nb, 2):
        whi[B * i : B * i + B, B * i + B : B * i + 2 * B] = zero
        wlo[B * i : B * i + B, B * i + B : B * i + 2 * B] = zero

    def block(i, k):
        at = panel_at(k) + B * i
        return gfull[at : at + B, :]

    def against(side, other, n):
        d = dot(thr[side, :, :n], rboth[other, :n, :]) + dot(tlr[side, :, :n], rboth[other, :n, :])
        return d[:, :B] + d[:, B:]

    def keep_r(side, i, r):
        ii = slice(B * i, B * i + B)
        hi, lo = halves(r)
        rboth[side, ii, :B] = hi
        rboth[side, ii, B:] = lo
        hi, lo = halves(r.T)
        thr[side, :, ii] = hi
        tlr[side, :, ii] = lo

    def row_of_w(k):
        ii = slice(B * k, B * k + B)

        def chunk(c, e):
            mh, ml = whi[ii, ii], wlo[ii, ii]
            th, tl = tk[0, :, c:e], tk[1, :, c:e]
            w = dot(jnp.concatenate([mh, ml], axis=1), jnp.concatenate([th, th], axis=0)) + dot(
                jnp.concatenate([mh, ml], axis=1), jnp.concatenate([tl, tl], axis=0))
            hi, lo = halves(-w)
            whi[ii, c:e] = hi
            wlo[ii, c:e] = lo

        return [functools.partial(chunk, c, min(c + 256, B * k)) for c in range(0, B * k, 256)]

    def t_of(k):
        n = B * k

        def chunk(c, e):
            th, tl = thr[k % 2, :, c:n], tlr[k % 2, :, c:n]
            t = dot(th, whi[c:n, c:e]) + (dot(tl, whi[c:n, c:e]) + dot(th, wlo[c:n, c:e]))
            hi, lo = halves(t)
            tk[0, :, c:e] = hi
            tk[1, :, c:e] = lo

        return [functools.partial(chunk, c, min(c + 256, n)) for c in range(0, n, 256)]

    def x_of(k):
        kk, m = slice(B * k, B * k + B), B * k + B

        def chunk(c):
            r = slice(c, c + rows // 4)
            x[r, kk] = dot_t(phi[r, :m], whi[kk, :m]) + (dot_t(plo[r, :m], whi[kk, :m]) + dot_t(phi[r, :m], wlo[kk, :m]))

        return [functools.partial(chunk, c) for c in range(0, rows, rows // 4)]

    def r_of(k):
        side, n = k % 2, B * (k - 1)

        def split():
            at = panel_at(k)
            hi, lo = halves(gfull[at : at + n, :])
            gboth[:n, :B] = hi
            gboth[:n, B:] = lo

        def one(i):
            ii, m = slice(B * i, B * i + B), B * i + B
            r = dot(whi[ii, :m], gboth[:m, :]) + dot(wlo[ii, :m], gboth[:m, :])
            keep_r(side, i, r[:, :B] + r[:, B:])

        def rest():
            b, d = block(k - 1, k), block(k, k)
            if n:
                b = b - against(1 - side, side, n)
                d = d - against(side, side, n)
            bd[0] = b
            bd[1] = d

        return ([split] if n else []) + [functools.partial(one, i) for i in range(k - 1)] + [rest]

    current = block(0, 0)
    for k in range(nb):
        jobs = []
        if k > 0:
            jobs += row_of_w(k - 1) + t_of(k)
        if k + 1 < nb and k + 1 not in LATE:
            jobs += r_of(k + 1)
        if k > 0:
            jobs += x_of(k - 1)
        every = max(1, 112 // (len(jobs) + 1))
        count = [0]

        def fill():
            count[0] += 1
            if count[0] % every == 0 and jobs:
                jobs.pop(0)()

        inv = diag_inverse(current, work, winv, fill)
        while jobs:
            jobs.pop(0)()
        kk = slice(B * k, B * k + B)
        hi, lo = halves(inv)
        whi[kk, kk] = hi
        wlo[kk, kk] = lo
        if k + 1 in LATE:
            after(k)
            for job in r_of(k + 1):
                job()
        if k + 1 < nb:
            side = (k + 1) % 2
            keep_r(side, k, dot(left_stack(inv), right_stack(bd[0])))
            d = dot(thr[side, :, kk], rboth[side, kk, :]) + dot(tlr[side, :, kk], rboth[side, kk, :])
            current = bd[1] - (d[:, :B] + d[:, B:])
        if k + 1 not in LATE:
            after(k)
    for job in row_of_w(nb - 1) + x_of(nb - 1):
        job()


def kernel(nb, stat, basis, out, stage, shi, slo, bbuf, pacc, pin, phi, plo, thi, tlo, gloc, gfull, ysum, rh, r1, r2,
           whi, wlo, x, work, winv, gboth, rboth, thr, tlr, tk, bd, ssem, bsem, xsend, xrecv, osend, orecv, asend, arecv):
    core = lax.axis_index("col")
    row = lax.axis_index("row")
    a, b = row // 4, row % 4
    mate = {"col": 1 - core}

    def along(first, d):
        if first:
            return a * 4 + (b + d) % 4
        return ((a + d) % 4) * 4 + b

    rows = phi.shape[0]
    half = rows // 2
    depth = basis.shape[1]
    nk = depth // KC

    def layer_of(i):
        return i * core + (1 - i) * (1 - core)

    def stat_copy(i, kc):
        ks = pl.ds(pl.multiple_of(kc * KC, 128), KC)
        return pltpu.make_async_copy(stat.at[layer_of(i), :, ks], stage.at[kc], ssem.at[kc])

    def basis_copy(i, q, kc, size):
        ks = pl.ds(pl.multiple_of(kc * size, 128), size)
        cols = pl.ds(pl.multiple_of(q * 256, 128), 256)
        return pltpu.make_async_copy(basis.at[layer_of(i), ks, cols], bbuf.at[i, ks, :], bsem.at[i, kc])

    for kc in range(nk):
        stat_copy(0, kc).start()
        basis_copy(0, 0, kc, KC).start()
    for kc in range(nk):
        basis_copy(1, 0, kc, KC).start()

    barrier = pltpu.get_barrier_semaphore()
    pl.semaphore_signal(barrier, inc=1, device_id=mate, device_id_type=MESH)
    for d in range(1, 4):
        pl.semaphore_signal(barrier, inc=1, device_id={"row": along(True, d)}, device_id_type=MESH)
        pl.semaphore_signal(barrier, inc=1, device_id={"row": along(False, d)}, device_id_type=MESH)
    pl.semaphore_wait(barrier, 7)

    def swap(q):
        return pltpu.make_async_remote_copy(
            src_ref=pacc.at[2 * q], dst_ref=pin.at[q],
            send_sem=xsend.at[q], recv_sem=xrecv.at[q], device_id=mate, device_id_type=MESH)

    def coords(k):
        return (b, a) if k % 2 == 0 else (a, b)

    def reduce_copies(k, s):
        kind = stages(k)[s]
        first = k % 2 == 0
        me1, me2 = coords(k)
        big, small = 32 * (k + 1), 8 * (k + 1)
        part = big // 2
        base = panel_at(k)

        def rows_of(chunk, size, shift=0):
            return pl.ds(pl.multiple_of(base + chunk % 4 * big + shift, 8), size)

        made = []
        for n, d in enumerate((1, 2, 3) if kind in ("all", "second", "spread2", "spread") else (1, 3)):
            peer = along(first, d)
            if kind == "all":
                src, dst = gloc.at[rows_of(me1 + d, big)], r1.at[n, pl.ds(base // 4, big)]
            elif kind == "half":
                src, dst = gloc.at[rows_of(me1 + 2, part, n * part)], rh.at[n, pl.ds(base // 8, part)]
            elif kind == "whole":
                src, dst = gloc.at[rows_of(me1 + d, big)], r1.at[n, pl.ds(base // 4, big)]
            elif kind == "second":
                at = pl.multiple_of(base // 4 + ((me2 + d) % 4) * small, 8)
                src, dst = ysum.at[pl.ds(at, small)], r2.at[n, pl.ds(base // 16, small)]
                peer = along(not first, d)
            elif kind == "spread2":
                at = pl.multiple_of(base + me1 * big + me2 * small, 8)
                src = dst = gfull.at[pl.ds(at, small)]
                peer = along(not first, d)
            elif kind in ("spread", "near"):
                src = dst = gfull.at[rows_of(me1, big)]
            else:
                src = dst = gfull.at[rows_of(me1 + 4 - d, part, n * part)]
            made.append(pltpu.make_async_remote_copy(
                src_ref=src, dst_ref=dst, send_sem=asend.at[k, s, n], recv_sem=arecv.at[k, s, n],
                device_id={"row": peer}, device_id_type=MESH))
        return made

    def begin(k, s):
        for c in reduce_copies(k, s):
            c.start()

    def event(k, s):
        me1, me2 = coords(k)
        big, small = 32 * (k + 1), 8 * (k + 1)
        base = panel_at(k)
        for c in reduce_copies(k, s - 1):
            c.wait_recv()
        done = stages(k)[s - 1]
        if done == "half":
            part = big // 2
            for way, d in enumerate((1, 3)):
                at = pl.multiple_of(base + (me1 + d) % 4 * big + way * part, 8)
                gloc[pl.ds(at, part), :] += rh[way, base // 8 : base // 8 + part, :]
        elif done in ("all", "whole"):
            at = pl.multiple_of(base + me1 * big, 8)
            here = slice(base // 4, base // 4 + big)
            total = gloc[pl.ds(at, big), :] + (r1[0, here, :] + r1[1, here, :])
            ysum[here, :] = total + r1[2, here, :] if done == "all" else total
        elif done == "second":
            at = pl.multiple_of(base // 4 + me2 * small, 8)
            here = slice(base // 16, base // 16 + small)
            to = pl.multiple_of(base + me1 * big + me2 * small, 8)
            gfull[pl.ds(to, small), :] = (ysum[pl.ds(at, small), :] + r2[0, here, :]) + (r2[1, here, :] + r2[2, here, :])
        if s < len(stages(k)):
            begin(k, s)

    def wave(*pairs):
        for q, s in pairs:
            event(2 * q, s)
            event(2 * q + 1, s)

    def gram(q):
        cols = slice(256 * q, 256 * q + 256)
        swap(q).wait_recv()
        prod = pacc[2 * q + 1] + pin[q]
        hi, lo = halves(prod)
        phi[:, cols] = hi
        plo[:, cols] = lo
        hi_t, lo_t = halves(prod.T)
        thi[cols, :] = hi_t
        tlo[cols, :] = lo_t
        e, o = panel_at(2 * q), panel_at(2 * q + 1)
        for i in range(0, 256 * q + 256, 256):
            ii = slice(i, i + 256)
            g = dot(thi[ii, :], hi) + (dot(tlo[ii, :], hi) + dot(thi[ii, :], lo))
            take = min(256, 256 * q + B - i)
            gloc[e + i : e + i + take, :] = g[:take, :B]
            gloc[o + i : o + i + 256, :] = g[:, B:]
        begin(2 * q, 0)
        begin(2 * q + 1, 0)

    for i in range(2):

        def first(kc, carry):
            stat_copy(i, kc).wait()
            basis_copy(i, 0, kc, KC).wait()
            ks = pl.ds(pl.multiple_of(kc * KC, 128), KC)
            hi, lo = halves(stage[kc])
            shi[i, :, ks] = hi
            slo[i, :, ks] = lo
            if i == 0:
                stat_copy(1, kc).start()
            bhi, blo = halves(bbuf[i, ks, :])
            r = dot(hi, bhi) + dot(lo, bhi) + dot(hi, blo)

            @pl.when(kc == 0)
            def _():
                pacc[i] = r

            @pl.when(kc > 0)
            def _():
                pacc[i] += r

            return carry

        lax.fori_loop(0, nk, first, 0)
        for kc in range(2):
            basis_copy(i, 1, kc, depth // 2).start()
        if i == 0:
            swap(0).start()
    gram(0)

    plan = {3: ((0, 1),), 4: ((0, 2),), 5: ((0, 3), (1, 1)), 6: ((1, 2), (2, 1)), 7: ((0, 4), (1, 3), (2, 2))}

    def column_step(t, carry):
        q, i = t // 2, t % 2
        for kc in range(2):
            basis_copy(i, q, kc, depth // 2).wait()
        acc = None
        for kc in range(2):
            ks = slice(kc * depth // 2, (kc + 1) * depth // 2)
            bhi, blo = halves(bbuf[i, ks, :])
            for left, right in ((shi, bhi), (slo, bhi), (shi, blo)):
                r = dot(left[i, :, ks], right)
                acc = r if acc is None else acc + r
        pacc[t] = acc

        @pl.when(t < 6)
        def _():
            for kc in range(2):
                basis_copy(i, q + 1, kc, depth // 2).start()

        for tt in range(2, 8):

            @pl.when(t == tt)
            def _():
                if tt % 2 == 0:
                    swap(tt // 2).start()
                wave(*plan.get(tt, ()))
                if tt % 2 == 1:
                    gram(tt // 2)

        return carry

    lax.fori_loop(2, 8, column_step, 0)

    late = {
        0: ((1, 4), (2, 3), (3, 1)), 1: ((2, 4), (3, 2)), 2: ((2, 5), (3, 3)), 3: ((2, 6), (3, 4)), 4: ((3, 5),), 5: ((3, 6),),
    }
    out_copies = []

    def give(q):
        cols = slice(256 * q, 256 * q + 256)
        c = pltpu.make_async_remote_copy(
            src_ref=x.at[pl.ds(pl.multiple_of((1 - core) * half, 8), half), cols],
            dst_ref=out.at[core, :, cols],
            send_sem=osend.at[q], recv_sem=orecv.at[q], device_id=mate, device_id_type=MESH)
        c.start()
        out_copies.append(c)
        out[core, :, cols] = x[pl.ds(pl.multiple_of(core * half, 8), half), cols]

    def after(k):
        wave(*late.get(k, ()))
        if k > 0 and k % 2 == 0:
            give(k // 2 - 1)

    factor_and_solve(nb, gfull, phi, plo, whi, wlo, x, work, winv, gboth, rboth, thr, tlr, tk, bd, after)
    give(nb // 2 - 1)

    for c in out_copies:
        c.wait()
    for q in range(nb // 2):
        swap(q).wait_send()
    for k in range(nb):
        for s in range(len(stages(k))):
            for c in reduce_copies(k, s):
                c.wait_send()


def refresh(statistic, eigenbasis):
    _, rows, depth = statistic.shape
    k = eigenbasis.shape[2]
    nb = k // B
    vm = pl.BlockSpec(memory_space=pltpu.VMEM)
    total = panel_at(nb)
    dma = pltpu.SemaphoreType.DMA
    return pl.pallas_call(
        functools.partial(kernel, nb),
        out_shape=jax.ShapeDtypeStruct((2, rows // 2, k), F32),
        in_specs=[pl.BlockSpec(memory_space=pl.ANY)] * 2,
        out_specs=vm,
        scratch_shapes=[
            pltpu.VMEM((depth // KC, rows, KC), F32),
            pltpu.VMEM((2, rows, depth), BF16),
            pltpu.VMEM((2, rows, depth), BF16),
            pltpu.VMEM((2, depth, 256), F32),
            pltpu.VMEM((8, rows, 256), F32),
            pltpu.VMEM((4, rows, 256), F32),
            pltpu.VMEM((rows, k), BF16),
            pltpu.VMEM((rows, k), BF16),
            pltpu.VMEM((k, rows), BF16),
            pltpu.VMEM((k, rows), BF16),
            pltpu.VMEM((total, B), F32),
            pltpu.VMEM((total, B), F32),
            pltpu.VMEM((total // 4, B), F32),
            pltpu.VMEM((2, total // 8, B), F32),
            pltpu.VMEM((3, total // 4, B), F32),
            pltpu.VMEM((3, total // 16, B), F32),
            pltpu.VMEM((k, k), BF16),
            pltpu.VMEM((k, k), BF16),
            pltpu.VMEM((rows, k), F32),
            pltpu.VMEM((B, B), F32),
            pltpu.VMEM((B, B), F32),
            pltpu.VMEM((k, 2 * B), BF16),
            pltpu.VMEM((2, k, 2 * B), BF16),
            pltpu.VMEM((2, B, k), BF16),
            pltpu.VMEM((2, B, k), BF16),
            pltpu.VMEM((2, B, k), BF16),
            pltpu.VMEM((2, B, B), F32),
            dma((depth // KC,)),
            dma((2, depth // KC)),
            dma((nb // 2,)),
            dma((nb // 2,)),
            dma((nb // 2,)),
            dma((nb // 2,)),
            dma((nb, 6, 3)),
            dma((nb, 6, 3)),
        ],
        compiler_params=pltpu.CompilerParams(
            vmem_limit_bytes=67043328, collective_id=0, has_side_effects=True),
        name="refresh",
    )(statistic, eigenbasis)


def solution(mesh):
    placed = (P("layer", "row", "col"), P("layer", "col", None))
    return jax.shard_map(
        refresh,
        mesh=mesh,
        in_specs=placed,
        out_specs=P("layer", ("row", "col"), None),
        check_vma=False,
    )
```

```python
import functools
import jax
import jax.numpy as jnp
from jax import lax
from jax.experimental import pallas as pl
from jax.experimental.pallas import tpu as pltpu
from jax.sharding import PartitionSpec as P

F32, BF16 = jnp.float32, jnp.bfloat16
MESH = pl.DeviceIdType.MESH
B = 128
KC = 512
RING = (2, 3)
LATE = (4, 6)
DIRECT_STAGES = ("all", "second", "spread2", "spread")
RING_STAGES = ("half", "whole", "second", "spread2", "near", "relay")


def stages(k):
    return RING_STAGES if k // 2 in RING else DIRECT_STAGES


def halves(x):
    hi = x.astype(BF16)
    lo = (x - hi.astype(F32)).astype(BF16)
    return hi, lo


def dot(a, b):
    return jnp.dot(a, b, preferred_element_type=F32)


def dot_t(a, b):
    return lax.dot_general(a, b, (((1,), (1,)), ((), ())), preferred_element_type=F32)


def left_stack(x):
    hi, lo = halves(x)
    return jnp.concatenate([hi, lo, hi, lo], axis=1)


def right_stack(x):
    hi, lo = halves(x)
    return jnp.concatenate([hi, hi, lo, lo], axis=0)


def spread(v, s):
    return jnp.broadcast_to(v[s : s + 1, :], (8, 128))


def factor_group(rows, inv, col0, wide, fill):
    n = len(rows)
    sub = lax.broadcasted_iota(jnp.int32, (8, 128), 0)
    for t in range(0, n, wide // 8):
        base = col0 + 8 * t
        cols = []
        for j in range(wide):
            col = {}
            for g in range(t + j // 8, n):
                c = jnp.broadcast_to(rows[g][:, base + j : base + j + 1], (8, 128))
                col[g] = c + 0.0 if g < t + wide // 8 else c
            cols.append(col)
        pivot = spread(cols[0][t], 0)
        scale = None
        for j in range(wide):
            gj, s = t + j // 8, j % 8
            mult = {g: c / pivot for g, c in cols[j].items()}
            across = {k: spread(cols[j][t + k // 8], k % 8) for k in range(j + 1, wide)}
            rs = lax.rsqrt(pivot)
            scale = rs if s == 0 else jnp.where(sub >= s, rs, scale)
            if j + 1 < wide:
                own = spread(cols[j + 1][t + (j + 1) // 8], (j + 1) % 8)
                pivot = own - (across[j + 1] * across[j + 1]) / pivot
            for k in range(j + 1, wide):
                for g in cols[k]:
                    cols[k][g] = cols[k][g] - mult[g] * across[k]
            mult[gj] = jnp.where(sub > s, mult[gj], 0.0)
            row, irow = spread(rows[gj], s), spread(inv[gj], s)
            for g in mult:
                rows[g] = rows[g] - mult[g] * row
                inv[g] = inv[g] - mult[g] * irow
            if s == 7:
                rows[gj] = rows[gj] * scale
                inv[gj] = inv[gj] * scale
            fill()
    return rows, inv


def diag_inverse(block, work, winv, fill, step=64, wide=16):
    r = lax.broadcasted_iota(jnp.int32, (B, B), 0)
    c = lax.broadcasted_iota(jnp.int32, (B, B), 1)
    work[...] = block
    winv[...] = jnp.where(r == c, 1.0, 0.0).astype(F32)
    for lo in range(0, B, step):
        rows = [work[lo + 8 * g : lo + 8 * g + 8, :] for g in range(step // 8)]
        inv = [winv[lo + 8 * g : lo + 8 * g + 8, :] for g in range(step // 8)]
        rows, inv = factor_group(rows, inv, lo, wide, fill)
        rfull = jnp.concatenate(rows, axis=0)
        ifull = jnp.concatenate(inv, axis=0)
        winv[lo : lo + step, :] = ifull
        if lo + step < B:
            both = right_stack(jnp.concatenate([rfull, ifull], axis=1))
            lt = left_stack(rfull.T)
            upd = dot(lt[lo + step :, :], both)
            work[lo + step :, :] -= upd[:, :B]
            winv[lo + step :, :] -= upd[:, B:]
    return winv[...]


def panel_at(k):
    return B * k * (k + 1) // 2


def factor_and_solve(nb, gfull, phi, plo, whi, wlo, x, work, winv, gboth, rboth, thr, tlr, tk, bd, after):
    rows = phi.shape[0]
    zero = jnp.zeros((B, B), BF16)
    for i in range(0, nb, 2):
        whi[B * i : B * i + B, B * i + B : B * i + 2 * B] = zero
        wlo[B * i : B * i + B, B * i + B : B * i + 2 * B] = zero

    def block(i, k):
        at = panel_at(k) + B * i
        return gfull[at : at + B, :]

    def against(side, other, n):
        d = dot(thr[side, :, :n], rboth[other, :n, :]) + dot(tlr[side, :, :n], rboth[other, :n, :])
        return d[:, :B] + d[:, B:]

    def keep_r(side, i, r):
        ii = slice(B * i, B * i + B)
        hi, lo = halves(r)
        rboth[side, ii, :B] = hi
        rboth[side, ii, B:] = lo
        hi, lo = halves(r.T)
        thr[side, :, ii] = hi
        tlr[side, :, ii] = lo

    def row_of_w(k):
        ii = slice(B * k, B * k + B)

        def chunk(c, e):
            mh, ml = whi[ii, ii], wlo[ii, ii]
            th, tl = tk[0, :, c:e], tk[1, :, c:e]
            w = dot(jnp.concatenate([mh, ml], axis=1), jnp.concatenate([th, th], axis=0)) + dot(
                jnp.concatenate([mh, ml], axis=1), jnp.concatenate([tl, tl], axis=0))
            hi, lo = halves(-w)
            whi[ii, c:e] = hi
            wlo[ii, c:e] = lo

        return [functools.partial(chunk, c, min(c + 256, B * k)) for c in range(0, B * k, 256)]

    def t_of(k):
        n = B * k

        def chunk(c, e):
            th, tl = thr[k % 2, :, c:n], tlr[k % 2, :, c:n]
            t = dot(th, whi[c:n, c:e]) + (dot(tl, whi[c:n, c:e]) + dot(th, wlo[c:n, c:e]))
            hi, lo = halves(t)
            tk[0, :, c:e] = hi
            tk[1, :, c:e] = lo

        return [functools.partial(chunk, c, min(c + 256, n)) for c in range(0, n, 256)]

    def x_of(k):
        kk, m = slice(B * k, B * k + B), B * k + B

        def chunk(c):
            r = slice(c, c + rows // 4)
            x[r, kk] = dot_t(phi[r, :m], whi[kk, :m]) + (dot_t(plo[r, :m], whi[kk, :m]) + dot_t(phi[r, :m], wlo[kk, :m]))

        return [functools.partial(chunk, c) for c in range(0, rows, rows // 4)]

    def r_of(k):
        side, n = k % 2, B * (k - 1)

        def split():
            at = panel_at(k)
            hi, lo = halves(gfull[at : at + n, :])
            gboth[:n, :B] = hi
            gboth[:n, B:] = lo

        def one(i):
            ii, m = slice(B * i, B * i + B), B * i + B
            r = dot(whi[ii, :m], gboth[:m, :]) + dot(wlo[ii, :m], gboth[:m, :])
            keep_r(side, i, r[:, :B] + r[:, B:])

        def rest():
            b, d = block(k - 1, k), block(k, k)
            if n:
                b = b - against(1 - side, side, n)
                d = d - against(side, side, n)
            bd[0] = b
            bd[1] = d

        return ([split] if n else []) + [functools.partial(one, i) for i in range(k - 1)] + [rest]

    current = block(0, 0)
    for k in range(nb):
        jobs = []
        if k > 0:
            jobs += row_of_w(k - 1) + t_of(k)
        if k + 1 < nb and k + 1 not in LATE:
            jobs += r_of(k + 1)
        if k > 0:
            jobs += x_of(k - 1)
        every = max(1, 112 // (len(jobs) + 1))
        count = [0]

        def fill():
            count[0] += 1
            if count[0] % every == 0 and jobs:
                jobs.pop(0)()

        inv = diag_inverse(current, work, winv, fill)
        while jobs:
            jobs.pop(0)()
        kk = slice(B * k, B * k + B)
        hi, lo = halves(inv)
        whi[kk, kk] = hi
        wlo[kk, kk] = lo
        if k + 1 in LATE:
            after(k)
            for job in r_of(k + 1):
                job()
        if k + 1 < nb:
            side = (k + 1) % 2
            keep_r(side, k, dot(left_stack(inv), right_stack(bd[0])))
            d = dot(thr[side, :, kk], rboth[side, kk, :]) + dot(tlr[side, :, kk], rboth[side, kk, :])
            current = bd[1] - (d[:, :B] + d[:, B:])
        if k + 1 not in LATE:
            after(k)
    for job in row_of_w(nb - 1) + x_of(nb - 1):
        job()


def kernel(nb, stat, basis, out, stage, shi, slo, bbuf, pacc, pin, phi, plo, thi, tlo, gloc, gfull, ysum, rh, r1, r2,
           whi, wlo, x, work, winv, gboth, rboth, thr, tlr, tk, bd, ssem, bsem, xsend, xrecv, osend, orecv, olocal, asend, arecv):
    core = lax.axis_index("col")
    row = lax.axis_index("row")
    a, b = row // 4, row % 4
    mate = {"col": 1 - core}

    def along(first, d):
        if first:
            return a * 4 + (b + d) % 4
        return ((a + d) % 4) * 4 + b

    rows = phi.shape[0]
    half = rows // 2
    depth = basis.shape[1]
    nk = depth // KC

    def layer_of(i):
        return i * core + (1 - i) * (1 - core)

    def stat_copy(i, kc):
        ks = pl.ds(pl.multiple_of(kc * KC, 128), KC)
        return pltpu.make_async_copy(stat.at[layer_of(i), :, ks], stage.at[kc], ssem.at[kc])

    def basis_copy(i, q, kc, size):
        ks = pl.ds(pl.multiple_of(kc * size, 128), size)
        cols = pl.ds(pl.multiple_of(q * 256, 128), 256)
        return pltpu.make_async_copy(basis.at[layer_of(i), ks, cols], bbuf.at[i, ks, :], bsem.at[i, kc])

    for kc in range(nk):
        stat_copy(0, kc).start()
        basis_copy(0, 0, kc, KC).start()
    for kc in range(nk):
        basis_copy(1, 0, kc, KC).start()

    barrier = pltpu.get_barrier_semaphore()
    pl.semaphore_signal(barrier, inc=1, device_id=mate, device_id_type=MESH)
    for d in range(1, 4):
        pl.semaphore_signal(barrier, inc=1, device_id={"row": along(True, d)}, device_id_type=MESH)
        pl.semaphore_signal(barrier, inc=1, device_id={"row": along(False, d)}, device_id_type=MESH)

    def swap(q):
        return pltpu.make_async_remote_copy(
            src_ref=pacc.at[2 * q], dst_ref=pin.at[q],
            send_sem=xsend.at[q], recv_sem=xrecv.at[q], device_id=mate, device_id_type=MESH)

    def coords(k):
        return (b, a) if k % 2 == 0 else (a, b)

    def reduce_copies(k, s):
        kind = stages(k)[s]
        first = k % 2 == 0
        me1, me2 = coords(k)
        big, small = 32 * (k + 1), 8 * (k + 1)
        part = big // 2
        base = panel_at(k)

        def rows_of(chunk, size, shift=0):
            return pl.ds(pl.multiple_of(base + chunk % 4 * big + shift, 8), size)

        made = []
        for n, d in enumerate((1, 2, 3) if kind in ("all", "second", "spread2", "spread") else (1, 3)):
            peer = along(first, d)
            if kind == "all":
                src, dst = gloc.at[rows_of(me1 + d, big)], r1.at[n, pl.ds(base // 4, big)]
            elif kind == "half":
                src, dst = gloc.at[rows_of(me1 + 2, part, n * part)], rh.at[n, pl.ds(base // 8, part)]
            elif kind == "whole":
                src, dst = gloc.at[rows_of(me1 + d, big)], r1.at[n, pl.ds(base // 4, big)]
            elif kind == "second":
                at = pl.multiple_of(base // 4 + ((me2 + d) % 4) * small, 8)
                src, dst = ysum.at[pl.ds(at, small)], r2.at[n, pl.ds(base // 16, small)]
                peer = along(not first, d)
            elif kind == "spread2":
                at = pl.multiple_of(base + me1 * big + me2 * small, 8)
                src = dst = gfull.at[pl.ds(at, small)]
                peer = along(not first, d)
            elif kind in ("spread", "near"):
                src = dst = gfull.at[rows_of(me1, big)]
            else:
                src = dst = gfull.at[rows_of(me1 + 4 - d, part, n * part)]
            made.append(pltpu.make_async_remote_copy(
                src_ref=src, dst_ref=dst, send_sem=asend.at[k, s, n], recv_sem=arecv.at[k, s, n],
                device_id={"row": peer}, device_id_type=MESH))
        return made

    def begin(k, s):
        for c in reduce_copies(k, s):
            c.start()

    def event(k, s):
        me1, me2 = coords(k)
        big, small = 32 * (k + 1), 8 * (k + 1)
        base = panel_at(k)
        for c in reduce_copies(k, s - 1):
            c.wait_recv()
        done = stages(k)[s - 1]
        if done == "half":
            part = big // 2
            for way, d in enumerate((1, 3)):
                at = pl.multiple_of(base + (me1 + d) % 4 * big + way * part, 8)
                gloc[pl.ds(at, part), :] += rh[way, base // 8 : base // 8 + part, :]
        elif done in ("all", "whole"):
            at = pl.multiple_of(base + me1 * big, 8)
            here = slice(base // 4, base // 4 + big)
            total = gloc[pl.ds(at, big), :] + (r1[0, here, :] + r1[1, here, :])
            ysum[here, :] = total + r1[2, here, :] if done == "all" else total
        elif done == "second":
            at = pl.multiple_of(base // 4 + me2 * small, 8)
            here = slice(base // 16, base // 16 + small)
            to = pl.multiple_of(base + me1 * big + me2 * small, 8)
            gfull[pl.ds(to, small), :] = (ysum[pl.ds(at, small), :] + r2[0, here, :]) + (r2[1, here, :] + r2[2, here, :])
        if s < len(stages(k)):
            begin(k, s)

    def wave(*pairs):
        for q, s in pairs:
            event(2 * q, s)
            event(2 * q + 1, s)

    def gram(q):
        cols = slice(256 * q, 256 * q + 256)
        swap(q).wait_recv()
        prod = pacc[2 * q + 1] + pin[q]
        hi, lo = halves(prod)
        phi[:, cols] = hi
        plo[:, cols] = lo
        hi_t, lo_t = halves(prod.T)
        thi[cols, :] = hi_t
        tlo[cols, :] = lo_t
        e, o = panel_at(2 * q), panel_at(2 * q + 1)
        for i in range(0, 256 * q + 256, 256):
            ii = slice(i, i + 256)
            g = dot(thi[ii, :], hi) + (dot(tlo[ii, :], hi) + dot(thi[ii, :], lo))
            take = min(256, 256 * q + B - i)
            gloc[e + i : e + i + take, :] = g[:take, :B]
            gloc[o + i : o + i + 256, :] = g[:, B:]
        begin(2 * q, 0)
        begin(2 * q + 1, 0)

    for i in range(2):

        def first(kc, carry):
            stat_copy(i, kc).wait()
            basis_copy(i, 0, kc, KC).wait()
            ks = pl.ds(pl.multiple_of(kc * KC, 128), KC)
            hi, lo = halves(stage[kc])
            shi[i, :, ks] = hi
            slo[i, :, ks] = lo
            if i == 0:
                stat_copy(1, kc).start()
            bhi, blo = halves(bbuf[i, ks, :])
            r = dot(hi, bhi) + dot(lo, bhi) + dot(hi, blo)

            @pl.when(kc == 0)
            def _():
                pacc[i] = r

            @pl.when(kc > 0)
            def _():
                pacc[i] += r

            return carry

        lax.fori_loop(0, nk, first, 0)
        for kc in range(2):
            basis_copy(i, 1, kc, depth // 2).start()
        if i == 0:
            pl.semaphore_wait(barrier, 7)
            swap(0).start()
    gram(0)

    plan = {3: ((0, 1),), 4: ((0, 2),), 5: ((0, 3), (1, 1)), 6: ((1, 2), (2, 1)), 7: ((0, 4), (1, 3), (2, 2))}

    def column_step(t, carry):
        q, i = t // 2, t % 2
        for kc in range(2):
            basis_copy(i, q, kc, depth // 2).wait()
        acc = None
        for kc in range(2):
            ks = slice(kc * depth // 2, (kc + 1) * depth // 2)
            bhi, blo = halves(bbuf[i, ks, :])
            for left, right in ((shi, bhi), (slo, bhi), (shi, blo)):
                r = dot(left[i, :, ks], right)
                acc = r if acc is None else acc + r
        pacc[t] = acc

        @pl.when(t < 6)
        def _():
            for kc in range(2):
                basis_copy(i, q + 1, kc, depth // 2).start()

        for tt in range(2, 8):

            @pl.when(t == tt)
            def _():
                if tt % 2 == 0:
                    swap(tt // 2).start()
                wave(*plan.get(tt, ()))
                if tt % 2 == 1:
                    gram(tt // 2)

        return carry

    lax.fori_loop(2, 8, column_step, 0)

    late = {
        0: ((3, 1), (2, 3), (1, 4)), 1: ((3, 2), (2, 4)), 2: ((3, 3), (2, 5)), 3: ((3, 4), (2, 6)), 4: ((3, 5),), 5: ((3, 6),),
    }
    out_copies = []

    def give(n, cols):
        theirs = pltpu.make_async_remote_copy(
            src_ref=x.at[pl.ds(pl.multiple_of((1 - core) * half, 8), half), cols],
            dst_ref=out.at[core, :, cols],
            send_sem=osend.at[n], recv_sem=orecv.at[n], device_id=mate, device_id_type=MESH)
        ours = pltpu.make_async_copy(
            x.at[pl.ds(pl.multiple_of(core * half, 8), half), cols], out.at[core, :, cols], olocal.at[n])
        theirs.start()
        ours.start()
        out_copies.append(theirs)
        out_copies.append(ours)

    def after(k):
        wave(*late.get(k, ()))
        if k > 0 and k % 2 == 0:
            give(k // 2 - 1, slice(B * (k - 2), B * k))
        if k == nb - 1:
            give(nb // 2 - 1, slice(B * (k - 1), B * k))

    factor_and_solve(nb, gfull, phi, plo, whi, wlo, x, work, winv, gboth, rboth, thr, tlr, tk, bd, after)
    give(nb // 2, slice(B * (nb - 1), B * nb))

    for c in out_copies:
        c.wait()
    for q in range(nb // 2):
        swap(q).wait_send()
    for k in range(nb):
        for s in range(len(stages(k))):
            for c in reduce_copies(k, s):
                c.wait_send()


def refresh(statistic, eigenbasis):
    _, rows, depth = statistic.shape
    k = eigenbasis.shape[2]
    nb = k // B
    total = panel_at(nb)
    dma = pltpu.SemaphoreType.DMA
    return pl.pallas_call(
        functools.partial(kernel, nb),
        out_shape=jax.ShapeDtypeStruct((2, rows // 2, k), F32),
        in_specs=[pl.BlockSpec(memory_space=pl.ANY)] * 2,
        out_specs=pl.BlockSpec(memory_space=pl.ANY),
        scratch_shapes=[
            pltpu.VMEM((depth // KC, rows, KC), F32),
            pltpu.VMEM((2, rows, depth), BF16),
            pltpu.VMEM((2, rows, depth), BF16),
            pltpu.VMEM((2, depth, 256), F32),
            pltpu.VMEM((8, rows, 256), F32),
            pltpu.VMEM((4, rows, 256), F32),
            pltpu.VMEM((rows, k), BF16),
            pltpu.VMEM((rows, k), BF16),
            pltpu.VMEM((k, rows), BF16),
            pltpu.VMEM((k, rows), BF16),
            pltpu.VMEM((total, B), F32),
            pltpu.VMEM((total, B), F32),
            pltpu.VMEM((total // 4, B), F32),
            pltpu.VMEM((2, total // 8, B), F32),
            pltpu.VMEM((3, total // 4, B), F32),
            pltpu.VMEM((3, total // 16, B), F32),
            pltpu.VMEM((k, k), BF16),
            pltpu.VMEM((k, k), BF16),
            pltpu.VMEM((rows, k), F32),
            pltpu.VMEM((B, B), F32),
            pltpu.VMEM((B, B), F32),
            pltpu.VMEM((k, 2 * B), BF16),
            pltpu.VMEM((2, k, 2 * B), BF16),
            pltpu.VMEM((2, B, k), BF16),
            pltpu.VMEM((2, B, k), BF16),
            pltpu.VMEM((2, B, k), BF16),
            pltpu.VMEM((2, B, B), F32),
            dma((depth // KC,)),
            dma((2, depth // KC)),
            dma((nb // 2,)),
            dma((nb // 2,)),
            dma((nb // 2 + 1,)),
            dma((nb // 2 + 1,)),
            dma((nb // 2 + 1,)),
            dma((nb, 6, 3)),
            dma((nb, 6, 3)),
        ],
        compiler_params=pltpu.CompilerParams(
            vmem_limit_bytes=67043328, collective_id=0, has_side_effects=True),
        name="refresh",
    )(statistic, eigenbasis)


def solution(mesh):
    placed = (P("layer", "row", "col"), P("layer", "col", None))
    return jax.shard_map(
        refresh,
        mesh=mesh,
        in_specs=placed,
        out_specs=P("layer", ("row", "col"), None),
        check_vma=False,
    )
```

```python
import functools
import jax
import jax.numpy as jnp
from jax import lax
from jax.experimental import pallas as pl
from jax.experimental.pallas import tpu as pltpu
from jax.sharding import PartitionSpec as P

F32, BF16 = jnp.float32, jnp.bfloat16
MESH = pl.DeviceIdType.MESH
B = 128
KC = 1792
RING = (2, 3)
LATE = (4, 6)
DIRECT_STAGES = ("all", "second", "spread2", "spread")
RING_STAGES = ("half", "whole", "second", "spread2", "near", "relay")


def stages(k):
    return RING_STAGES if k // 2 in RING else DIRECT_STAGES


def halves(x):
    hi = x.astype(BF16)
    lo = (x - hi.astype(F32)).astype(BF16)
    return hi, lo


def dot(a, b):
    return jnp.dot(a, b, preferred_element_type=F32)


def dot_t(a, b):
    return lax.dot_general(a, b, (((1,), (1,)), ((), ())), preferred_element_type=F32)


def left_stack(x):
    hi, lo = halves(x)
    return jnp.concatenate([hi, lo, hi, lo], axis=1)


def right_stack(x):
    hi, lo = halves(x)
    return jnp.concatenate([hi, hi, lo, lo], axis=0)


def spread(v, s):
    return jnp.broadcast_to(v[s : s + 1, :], (8, 128))


def factor_group(rows, inv, col0, wide, fill):
    n = len(rows)
    sub = lax.broadcasted_iota(jnp.int32, (8, 128), 0)
    for t in range(0, n, wide // 8):
        base = col0 + 8 * t
        cols = []
        for j in range(wide):
            col = {}
            for g in range(t + j // 8, n):
                c = jnp.broadcast_to(rows[g][:, base + j : base + j + 1], (8, 128))
                col[g] = c + 0.0 if g < t + wide // 8 else c
            cols.append(col)
        pivot = spread(cols[0][t], 0)
        scale = None
        for j in range(wide):
            gj, s = t + j // 8, j % 8
            mult = {g: c / pivot for g, c in cols[j].items()}
            across = {k: spread(cols[j][t + k // 8], k % 8) for k in range(j + 1, wide)}
            rs = lax.rsqrt(pivot)
            scale = rs if s == 0 else jnp.where(sub >= s, rs, scale)
            if j + 1 < wide:
                own = spread(cols[j + 1][t + (j + 1) // 8], (j + 1) % 8)
                pivot = own - (across[j + 1] * across[j + 1]) / pivot
            for k in range(j + 1, wide):
                for g in cols[k]:
                    cols[k][g] = cols[k][g] - mult[g] * across[k]
            mult[gj] = jnp.where(sub > s, mult[gj], 0.0)
            row, irow = spread(rows[gj], s), spread(inv[gj], s)
            for g in mult:
                rows[g] = rows[g] - mult[g] * row
                inv[g] = inv[g] - mult[g] * irow
            if s == 7:
                rows[gj] = rows[gj] * scale
                inv[gj] = inv[gj] * scale
            fill()
    return rows, inv


def diag_inverse(block, work, winv, fill, step=64, wide=16):
    r = lax.broadcasted_iota(jnp.int32, (B, B), 0)
    c = lax.broadcasted_iota(jnp.int32, (B, B), 1)
    work[...] = block
    winv[...] = jnp.where(r == c, 1.0, 0.0).astype(F32)
    for lo in range(0, B, step):
        rows = [work[lo + 8 * g : lo + 8 * g + 8, :] for g in range(step // 8)]
        inv = [winv[lo + 8 * g : lo + 8 * g + 8, :] for g in range(step // 8)]
        rows, inv = factor_group(rows, inv, lo, wide, fill)
        rfull = jnp.concatenate(rows, axis=0)
        ifull = jnp.concatenate(inv, axis=0)
        winv[lo : lo + step, :] = ifull
        if lo + step < B:
            both = right_stack(jnp.concatenate([rfull, ifull], axis=1))
            lt = left_stack(rfull.T)
            upd = dot(lt[lo + step :, :], both)
            work[lo + step :, :] -= upd[:, :B]
            winv[lo + step :, :] -= upd[:, B:]
    return winv[...]


def panel_at(k):
    return B * k * (k + 1) // 2


def factor_and_solve(nb, gfull, phi, plo, whi, wlo, x, work, winv, gboth, rboth, thr, tlr, tk, bd, after):
    rows = phi.shape[0]
    zero = jnp.zeros((B, B), BF16)
    for i in range(0, nb, 2):
        whi[B * i : B * i + B, B * i + B : B * i + 2 * B] = zero
        wlo[B * i : B * i + B, B * i + B : B * i + 2 * B] = zero

    def block(i, k):
        at = panel_at(k) + B * i
        return gfull[at : at + B, :]

    def against(side, other, n):
        d = dot(thr[side, :, :n], rboth[other, :n, :]) + dot(tlr[side, :, :n], rboth[other, :n, :])
        return d[:, :B] + d[:, B:]

    def keep_r(side, i, r):
        ii = slice(B * i, B * i + B)
        hi, lo = halves(r)
        rboth[side, ii, :B] = hi
        rboth[side, ii, B:] = lo
        hi, lo = halves(r.T)
        thr[side, :, ii] = hi
        tlr[side, :, ii] = lo

    def row_of_w(k):
        ii = slice(B * k, B * k + B)

        def chunk(c, e):
            mh, ml = whi[ii, ii], wlo[ii, ii]
            th, tl = tk[0, :, c:e], tk[1, :, c:e]
            w = dot(jnp.concatenate([mh, ml], axis=1), jnp.concatenate([th, th], axis=0)) + dot(
                jnp.concatenate([mh, ml], axis=1), jnp.concatenate([tl, tl], axis=0))
            hi, lo = halves(-w)
            whi[ii, c:e] = hi
            wlo[ii, c:e] = lo

        return [functools.partial(chunk, c, min(c + 256, B * k)) for c in range(0, B * k, 256)]

    def t_of(k):
        n = B * k

        def chunk(c, e):
            th, tl = thr[k % 2, :, c:n], tlr[k % 2, :, c:n]
            t = dot(th, whi[c:n, c:e]) + (dot(tl, whi[c:n, c:e]) + dot(th, wlo[c:n, c:e]))
            hi, lo = halves(t)
            tk[0, :, c:e] = hi
            tk[1, :, c:e] = lo

        return [functools.partial(chunk, c, min(c + 256, n)) for c in range(0, n, 256)]

    def x_of(k):
        kk, m = slice(B * k, B * k + B), B * k + B

        def chunk(c):
            r = slice(c, c + rows // 4)
            x[r, kk] = dot_t(phi[r, :m], whi[kk, :m]) + (dot_t(plo[r, :m], whi[kk, :m]) + dot_t(phi[r, :m], wlo[kk, :m]))

        return [functools.partial(chunk, c) for c in range(0, rows, rows // 4)]

    def r_of(k):
        side, n = k % 2, B * (k - 1)

        def split():
            at = panel_at(k)
            hi, lo = halves(gfull[at : at + n, :])
            gboth[:n, :B] = hi
            gboth[:n, B:] = lo

        def one(i):
            ii, m = slice(B * i, B * i + B), B * i + B
            r = dot(whi[ii, :m], gboth[:m, :]) + dot(wlo[ii, :m], gboth[:m, :])
            keep_r(side, i, r[:, :B] + r[:, B:])

        def rest():
            b, d = block(k - 1, k), block(k, k)
            if n:
                b = b - against(1 - side, side, n)
                d = d - against(side, side, n)
            bd[0] = b
            bd[1] = d

        return ([split] if n else []) + [functools.partial(one, i) for i in range(k - 1)] + [rest]

    current = block(0, 0)
    for k in range(nb):
        jobs = []
        if k > 0:
            jobs += row_of_w(k - 1) + t_of(k)
        if k + 1 < nb and k + 1 not in LATE:
            jobs += r_of(k + 1)
        if k > 0:
            jobs += x_of(k - 1)
        every = max(1, 112 // (len(jobs) + 1))
        count = [0]

        def fill():
            count[0] += 1
            if count[0] % every == 0 and jobs:
                jobs.pop(0)()

        inv = diag_inverse(current, work, winv, fill)
        while jobs:
            jobs.pop(0)()
        kk = slice(B * k, B * k + B)
        hi, lo = halves(inv)
        whi[kk, kk] = hi
        wlo[kk, kk] = lo
        if k + 1 in LATE:
            after(k)
            for job in r_of(k + 1):
                job()
        if k + 1 < nb:
            side = (k + 1) % 2
            keep_r(side, k, dot(left_stack(inv), right_stack(bd[0])))
            d = dot(thr[side, :, kk], rboth[side, kk, :]) + dot(tlr[side, :, kk], rboth[side, kk, :])
            current = bd[1] - (d[:, :B] + d[:, B:])
        if k + 1 not in LATE:
            after(k)
    for job in row_of_w(nb - 1) + x_of(nb - 1):
        job()


def kernel(nb, stat, basis, out, stage, shi, slo, bbuf, pacc, pin, phi, plo, thi, tlo, gloc, gfull, ysum, rh, r1, r2,
           whi, wlo, x, work, winv, gboth, rboth, thr, tlr, tk, bd, ssem, bsem, xsend, xrecv, osend, orecv, olocal, asend, arecv):
    core = lax.axis_index("col")
    row = lax.axis_index("row")
    a, b = row // 4, row % 4
    mate = {"col": 1 - core}

    def along(first, d):
        if first:
            return a * 4 + (b + d) % 4
        return ((a + d) % 4) * 4 + b

    rows = phi.shape[0]
    half = rows // 2
    depth = basis.shape[1]
    nk = depth // KC

    def layer_of(i):
        return i * core + (1 - i) * (1 - core)

    def stat_copy(i, kc):
        ks = pl.ds(pl.multiple_of(kc * KC, 128), KC)
        return pltpu.make_async_copy(stat.at[layer_of(i), :, ks], stage.at[kc], ssem.at[kc])

    def basis_copy(i, q, kc, size):
        ks = pl.ds(pl.multiple_of(kc * size, 128), size)
        cols = pl.ds(pl.multiple_of(q * 256, 128), 256)
        return pltpu.make_async_copy(basis.at[layer_of(i), ks, cols], bbuf.at[i, ks, :], bsem.at[i, kc])

    for kc in range(nk):
        stat_copy(0, kc).start()
        basis_copy(0, 0, kc, KC).start()
    for kc in range(nk):
        basis_copy(1, 0, kc, KC).start()

    barrier = pltpu.get_barrier_semaphore()
    pl.semaphore_signal(barrier, inc=1, device_id=mate, device_id_type=MESH)
    for d in range(1, 4):
        pl.semaphore_signal(barrier, inc=1, device_id={"row": along(True, d)}, device_id_type=MESH)
        pl.semaphore_signal(barrier, inc=1, device_id={"row": along(False, d)}, device_id_type=MESH)

    def swap(q):
        return pltpu.make_async_remote_copy(
            src_ref=pacc.at[2 * q], dst_ref=pin.at[q],
            send_sem=xsend.at[q], recv_sem=xrecv.at[q], device_id=mate, device_id_type=MESH)

    def coords(k):
        return (b, a) if k % 2 == 0 else (a, b)

    def reduce_copies(k, s):
        kind = stages(k)[s]
        first = k % 2 == 0
        me1, me2 = coords(k)
        big, small = 32 * (k + 1), 8 * (k + 1)
        part = big // 2
        base = panel_at(k)

        def rows_of(chunk, size, shift=0):
            return pl.ds(pl.multiple_of(base + chunk % 4 * big + shift, 8), size)

        made = []
        for n, d in enumerate((1, 2, 3) if kind in ("all", "second", "spread2", "spread") else (1, 3)):
            peer = along(first, d)
            if kind == "all":
                src, dst = gloc.at[rows_of(me1 + d, big)], r1.at[n, pl.ds(base // 4, big)]
            elif kind == "half":
                src, dst = gloc.at[rows_of(me1 + 2, part, n * part)], rh.at[n, pl.ds(base // 8, part)]
            elif kind == "whole":
                src, dst = gloc.at[rows_of(me1 + d, big)], r1.at[n, pl.ds(base // 4, big)]
            elif kind == "second":
                at = pl.multiple_of(base // 4 + ((me2 + d) % 4) * small, 8)
                src, dst = ysum.at[pl.ds(at, small)], r2.at[n, pl.ds(base // 16, small)]
                peer = along(not first, d)
            elif kind == "spread2":
                at = pl.multiple_of(base + me1 * big + me2 * small, 8)
                src = dst = gfull.at[pl.ds(at, small)]
                peer = along(not first, d)
            elif kind in ("spread", "near"):
                src = dst = gfull.at[rows_of(me1, big)]
            else:
                src = dst = gfull.at[rows_of(me1 + 4 - d, part, n * part)]
            made.append(pltpu.make_async_remote_copy(
                src_ref=src, dst_ref=dst, send_sem=asend.at[k, s, n], recv_sem=arecv.at[k, s, n],
                device_id={"row": peer}, device_id_type=MESH))
        return made

    def begin(k, s):
        for c in reduce_copies(k, s):
            c.start()

    def event(k, s):
        me1, me2 = coords(k)
        big, small = 32 * (k + 1), 8 * (k + 1)
        base = panel_at(k)
        for c in reduce_copies(k, s - 1):
            c.wait_recv()
        done = stages(k)[s - 1]
        if done == "half":
            part = big // 2
            for way, d in enumerate((1, 3)):
                at = pl.multiple_of(base + (me1 + d) % 4 * big + way * part, 8)
                gloc[pl.ds(at, part), :] += rh[way, base // 8 : base // 8 + part, :]
        elif done in ("all", "whole"):
            at = pl.multiple_of(base + me1 * big, 8)
            here = slice(base // 4, base // 4 + big)
            total = gloc[pl.ds(at, big), :] + (r1[0, here, :] + r1[1, here, :])
            ysum[here, :] = total + r1[2, here, :] if done == "all" else total
        elif done == "second":
            at = pl.multiple_of(base // 4 + me2 * small, 8)
            here = slice(base // 16, base // 16 + small)
            to = pl.multiple_of(base + me1 * big + me2 * small, 8)
            gfull[pl.ds(to, small), :] = (ysum[pl.ds(at, small), :] + r2[0, here, :]) + (r2[1, here, :] + r2[2, here, :])
        if s < len(stages(k)):
            begin(k, s)

    def wave(*pairs):
        for q, s in pairs:
            event(2 * q, s)
            event(2 * q + 1, s)

    def gram(q):
        cols = slice(256 * q, 256 * q + 256)
        swap(q).wait_recv()
        prod = pacc[2 * q + 1] + pin[q]
        hi, lo = halves(prod)
        phi[:, cols] = hi
        plo[:, cols] = lo
        hi_t, lo_t = halves(prod.T)
        thi[cols, :] = hi_t
        tlo[cols, :] = lo_t
        e, o = panel_at(2 * q), panel_at(2 * q + 1)
        for i in range(0, 256 * q + 256, 256):
            ii = slice(i, i + 256)
            g = dot(thi[ii, :], hi) + (dot(tlo[ii, :], hi) + dot(thi[ii, :], lo))
            take = min(256, 256 * q + B - i)
            gloc[e + i : e + i + take, :] = g[:take, :B]
            gloc[o + i : o + i + 256, :] = g[:, B:]
        begin(2 * q, 0)
        begin(2 * q + 1, 0)

    for i in range(2):

        def first(kc, carry):
            stat_copy(i, kc).wait()
            basis_copy(i, 0, kc, KC).wait()
            ks = pl.ds(pl.multiple_of(kc * KC, 128), KC)
            hi, lo = halves(stage[kc])
            shi[i, :, ks] = hi
            slo[i, :, ks] = lo
            if i == 0:
                stat_copy(1, kc).start()
            bhi, blo = halves(bbuf[i, ks, :])
            r = dot(hi, bhi) + dot(lo, bhi) + dot(hi, blo)

            @pl.when(kc == 0)
            def _():
                pacc[i] = r

            @pl.when(kc > 0)
            def _():
                pacc[i] += r

            return carry

        lax.fori_loop(0, nk, first, 0)
        for kc in range(2):
            basis_copy(i, 1, kc, depth // 2).start()
        if i == 0:
            pl.semaphore_wait(barrier, 7)
            swap(0).start()
    gram(0)

    plan = {3: ((0, 1),), 4: ((0, 2),), 5: ((0, 3), (1, 1)), 6: ((1, 2), (2, 1)), 7: ((0, 4), (1, 3), (2, 2))}

    def column_step(t, carry):
        q, i = t // 2, t % 2
        for kc in range(2):
            basis_copy(i, q, kc, depth // 2).wait()
        acc = None
        for kc in range(2):
            ks = slice(kc * depth // 2, (kc + 1) * depth // 2)
            bhi, blo = halves(bbuf[i, ks, :])
            for left, right in ((shi, bhi), (slo, bhi), (shi, blo)):
                r = dot(left[i, :, ks], right)
                acc = r if acc is None else acc + r
        pacc[t] = acc

        @pl.when(t < 6)
        def _():
            for kc in range(2):
                basis_copy(i, q + 1, kc, depth // 2).start()

        for tt in range(2, 8):

            @pl.when(t == tt)
            def _():
                if tt % 2 == 0:
                    swap(tt // 2).start()
                wave(*plan.get(tt, ()))
                if tt % 2 == 1:
                    gram(tt // 2)

        return carry

    lax.fori_loop(2, 8, column_step, 0)

    late = {
        0: ((3, 1), (2, 3), (1, 4)), 1: ((3, 2), (2, 4)), 2: ((3, 3), (2, 5)), 3: ((3, 4), (2, 6)), 4: ((3, 5),), 5: ((3, 6),),
    }
    out_copies = []

    def give(n, cols):
        theirs = pltpu.make_async_remote_copy(
            src_ref=x.at[pl.ds(pl.multiple_of((1 - core) * half, 8), half), cols],
            dst_ref=out.at[core, :, cols],
            send_sem=osend.at[n], recv_sem=orecv.at[n], device_id=mate, device_id_type=MESH)
        ours = pltpu.make_async_copy(
            x.at[pl.ds(pl.multiple_of(core * half, 8), half), cols], out.at[core, :, cols], olocal.at[n])
        theirs.start()
        ours.start()
        out_copies.append(theirs)
        out_copies.append(ours)

    def after(k):
        wave(*late.get(k, ()))
        if k > 0 and k % 2 == 0:
            give(k // 2 - 1, slice(B * (k - 2), B * k))
        if k == nb - 1:
            give(nb // 2 - 1, slice(B * (k - 1), B * k))

    factor_and_solve(nb, gfull, phi, plo, whi, wlo, x, work, winv, gboth, rboth, thr, tlr, tk, bd, after)
    give(nb // 2, slice(B * (nb - 1), B * nb))

    for c in out_copies:
        c.wait()
    for q in range(nb // 2):
        swap(q).wait_send()
    for k in range(nb):
        for s in range(len(stages(k))):
            for c in reduce_copies(k, s):
                c.wait_send()


def refresh(statistic, eigenbasis):
    _, rows, depth = statistic.shape
    k = eigenbasis.shape[2]
    nb = k // B
    total = panel_at(nb)
    dma = pltpu.SemaphoreType.DMA
    return pl.pallas_call(
        functools.partial(kernel, nb),
        out_shape=jax.ShapeDtypeStruct((2, rows // 2, k), F32),
        in_specs=[pl.BlockSpec(memory_space=pl.ANY)] * 2,
        out_specs=pl.BlockSpec(memory_space=pl.ANY),
        scratch_shapes=[
            pltpu.VMEM((depth // KC, rows, KC), F32),
            pltpu.VMEM((2, rows, depth), BF16),
            pltpu.VMEM((2, rows, depth), BF16),
            pltpu.VMEM((2, depth, 256), F32),
            pltpu.VMEM((8, rows, 256), F32),
            pltpu.VMEM((4, rows, 256), F32),
            pltpu.VMEM((rows, k), BF16),
            pltpu.VMEM((rows, k), BF16),
            pltpu.VMEM((k, rows), BF16),
            pltpu.VMEM((k, rows), BF16),
            pltpu.VMEM((total, B), F32),
            pltpu.VMEM((total, B), F32),
            pltpu.VMEM((total // 4, B), F32),
            pltpu.VMEM((2, total // 8, B), F32),
            pltpu.VMEM((3, total // 4, B), F32),
            pltpu.VMEM((3, total // 16, B), F32),
            pltpu.VMEM((k, k), BF16),
            pltpu.VMEM((k, k), BF16),
            pltpu.VMEM((rows, k), F32),
            pltpu.VMEM((B, B), F32),
            pltpu.VMEM((B, B), F32),
            pltpu.VMEM((k, 2 * B), BF16),
            pltpu.VMEM((2, k, 2 * B), BF16),
            pltpu.VMEM((2, B, k), BF16),
            pltpu.VMEM((2, B, k), BF16),
            pltpu.VMEM((2, B, k), BF16),
            pltpu.VMEM((2, B, B), F32),
            dma((depth // KC,)),
            dma((2, depth // KC)),
            dma((nb // 2,)),
            dma((nb // 2,)),
            dma((nb // 2 + 1,)),
            dma((nb // 2 + 1,)),
            dma((nb // 2 + 1,)),
            dma((nb, 6, 3)),
            dma((nb, 6, 3)),
        ],
        compiler_params=pltpu.CompilerParams(
            vmem_limit_bytes=67043328, collective_id=0, has_side_effects=True),
        name="refresh",
    )(statistic, eigenbasis)


def solution(mesh):
    placed = (P("layer", "row", "col"), P("layer", "col", None))
    return jax.shard_map(
        refresh,
        mesh=mesh,
        in_specs=placed,
        out_specs=P("layer", ("row", "col"), None),
        check_vma=False,
    )
```
